32 devices in a mesh: exp: 8 (over z, x), head: 4 (over y, core).
Axes of the slice: x: 2, y: 2, z: 4, core: 2. Of those that a mesh axis runs over, the one named last changes fastest.
Arguments:
- normed_input: bfloat16 [8, 32, 4096], P('exp', None, 'head'), may hold values from -11 to 11
- norm_gain: float32 [4096], P('head'), may hold values from 0.5 to 1.5
- norm_scale: float32 [8, 32], P('exp'), may hold values from 0.4 to 4
- out_grad: bfloat16 [8, 32, 4096], P('exp', None, 'head'), may hold values from -6 to 6
- router_weight: bfloat16 [4096, 16], P('head'), may hold values from -0.125 to 0.125
- routed_experts: int32 [8, 32, 8], P('exp'), may hold values from 0 to 15, all different within a row; in each aligned block of 32 rows (0 to 31, 32 to 63, ..., all dimensions but the last counted through in order) at most 30 rows name the same one
- expert_grad: bfloat16 [16, 8, 30, 4096], P('exp', None, None, 'head'), may hold values from -10 to 10, as said below
- gate_grad: bfloat16 [16, 8, 30], P('exp'), may hold values from -48 to 48
- out_proj: bfloat16 [8192, 4096], P('head'), may hold values from -0.0625 to 0.0625
- query_states: bfloat16 [8, 32, 8192], P('exp', None, 'head'), may hold values from -5 to 5
- rotated_keys: bfloat16 [8, 32, 512], P('exp'), may hold values from -5 to 5
- value_tensor: bfloat16 [8, 32, 512], P('exp'), may hold values from -6 to 6
Outputs:
- grad_hidden: bfloat16 [8, 32, 4096], P('exp', None, 'head')
- grad_query: bfloat16 [8, 32, 8192], P('exp', 'head')
- key_gradient: bfloat16 [8, 32, 512], P('exp', 'head')
- value_gradient: bfloat16 [8, 32, 512], P('exp', 'head')
The draws below stay inside these ranges and needn't reach their ends.
Inputs may be any that keep to these rules, and one draw needn't show every extreme that they name: `routed_experts`: each token names 8 different experts. Within one sequence, an aligned block of 32 rows, no expert is named by more than 30 tokens, a bound that some block reaches. `expert_grad`: slot c of expert e for sequence s holds the row of the c-th token of sequence s, in order of position, that names e; slots past that count hold unrelated values. `gate_grad`: same slot layout as expert_grad.
All inputs are finite; a program needn't handle non-finite values.
Results may differ from the reference program's by a relative error of at most 0.01225.
Values may be sent and summed in bfloat16 or wider, within the bound.
A program may use at most 64 MiB of HBM per device.

```python
import math
import jax
import jax.numpy as jnp
import numpy as np
from jax import lax

D = 4096
QUERY_HEADS = 64
KEY_VALUE_HEADS = 4
HEAD_WIDTH = 128
TOPK = 8
EXPERTS = 16
SEQUENCE_COUNT = 8
SEQUENCE_TOKENS = 32
CAP = 30
N_HEAD = 4


def shared_rows(key):
    random_subkeys = jax.random.split(jax.random.fold_in(key, 101), 6)
    column_ramp = 0.5 + 1.5 * jnp.arange(D, dtype=jnp.float32) / D
    common = jnp.clip(jax.random.normal(random_subkeys[0], (D,), jnp.float32), -3.0, 3.0) * column_ramp
    return (random_subkeys, common)


def draw_normed_input(key, part):
    random_subkeys, common = shared_rows(key)
    base_rows = jnp.clip(jax.random.normal(random_subkeys[1], (SEQUENCE_COUNT, SEQUENCE_TOKENS, D), jnp.float32), -4.0, 4.0)
    drawn_rows = base_rows + 0.8 * common
    return drawn_rows.astype(jnp.bfloat16)


def draw_router_weight(key, part):
    random_subkeys, common = shared_rows(key)
    noise_part = jnp.clip(jax.random.normal(random_subkeys[3], (D, EXPERTS), jnp.float32), -4.0, 4.0)
    drawn_rows = noise_part * D ** (-0.5)
    return drawn_rows.astype(jnp.bfloat16)


def draw_expert_grad(key, part):
    random_subkeys, common = shared_rows(key)
    noise_part = jnp.clip(jax.random.normal(random_subkeys[5], (EXPERTS, SEQUENCE_COUNT, CAP, D), jnp.float32), -4.0, 4.0)
    drawn_rows = noise_part + 0.6 * common
    return drawn_rows.astype(jnp.bfloat16)


def attention_pair(key):
    random_subkeys = jax.random.split(jax.random.fold_in(key, 202), 2)
    queries = jnp.clip(jax.random.normal(random_subkeys[0], (SEQUENCE_COUNT, SEQUENCE_TOKENS, QUERY_HEADS * HEAD_WIDTH), jnp.float32), -4.0, 4.0)
    random_keyset = jnp.clip(jax.random.normal(random_subkeys[1], (SEQUENCE_COUNT, SEQUENCE_TOKENS, KEY_VALUE_HEADS * HEAD_WIDTH), jnp.float32), -4.0, 4.0)
    return (queries, random_keyset)


def draw_query_states(key, part):
    queries, random_keyset = attention_pair(key)
    return queries.astype(jnp.bfloat16)


def draw_rotated_keys(key, part):
    queries, random_keyset = attention_pair(key)
    return random_keyset.astype(jnp.bfloat16)


def steps_of(own_key, shape, cuts, smallest, largest):
    def one(dim, blocks):
        heights = jax.random.uniform(jax.random.fold_in(jax.random.fold_in(own_key, 6), dim), (blocks,), jnp.float32, smallest / len(cuts), largest / len(cuts))
        return jnp.repeat(jnp.exp(heights), shape[dim] // blocks).reshape((-1,) + (1,) * (len(shape) - dim - 1))

    factor_of = one(*cuts[0])
    for cut in cuts[1:]:
        factor_of = factor_of * one(*cut)
    return factor_of


def shared_out(own_key, own, number, rows, number_of, top, limit, slope):
    order = jax.random.permutation(own_key, number_of)
    crowded, ordinary = portions_of(number_of, rows * top, limit, slope, True), portions_of(number_of, rows * top, limit, slope, False)
    places = jnp.arange(number_of)

    def named(sizes, turn):
        used = int((sizes > 0).sum())
        fixed = max(1, used // 4)
        moved = fixed + (places - fixed + turn * (used - fixed)) % max(1, number_of - fixed)
        return jnp.zeros((number_of,), jnp.int32).at[order[jnp.where(places < fixed, places, moved)]].set(jnp.asarray(sizes, jnp.int32))

    sizes = jnp.where(number % 4 == 0, named(crowded, number // 4), named(ordinary, number - number // 4 - 1))
    mixed = jax.random.permutation(jax.random.fold_in(own, 3), number_of)
    source_of, taker = mixed[0:number_of // 2 * 2:2], mixed[1:number_of // 2 * 2:2]
    margin = jnp.minimum(sizes[source_of] - 1, limit - sizes[taker]) // 2
    margin = jnp.where((source_of == order[0]) | (taker == order[0]) | (sizes[taker] == 0), 0, jnp.maximum(margin, 0))
    moved = jax.random.randint(jax.random.fold_in(own, 4), (number_of // 2,), 0, 1 << 20) % (margin + 1)
    sizes = sizes.at[source_of].add(-moved).at[taker].add(moved)
    labels = jnp.searchsorted(jnp.cumsum(sizes), jnp.arange(rows * top), side="right").astype(jnp.int32)
    listing = labels.reshape(top, rows).T
    listing = listing[jax.random.permutation(jax.random.fold_in(own, 1), rows)]
    turn = jax.random.randint(jax.random.fold_in(own, 2), (rows, 1), 0, top)
    return jnp.take_along_axis(listing, (jnp.arange(top)[None, :] + turn) % top, axis=1)


def portions_of(count, total, most, skew, full):
    weights = [(1 << 20) // math.isqrt(rank ** skew) + 1 for rank in range(1, count + 1)]
    largest = most if full else min(most, max(-(-total // count), total * weights[0] // sum(weights)))
    least = 1 if total - largest >= count - 1 else 0
    counts, spare = [largest] + [least] * (count - 1), total - largest - least * (count - 1)
    while spare > 0:
        candidates = [i for i in range(1, count) if counts[i] < largest] or [i for i in range(1, count) if counts[i] < most]
        pool, left = sum([weights[i] for i in candidates]), spare
        for i in candidates:
            addition = min(most - counts[i], max(1, left * weights[i] // pool), spare)
            counts[i] = counts[i] + addition
            spare = spare - addition
    return np.array(counts)


def bell_draw(key, shape, scale, reach, pieces=(), held_as=jnp.bfloat16):
    entries = scale * jax.random.normal(key, shape, jnp.float32)
    if pieces:
        entries = entries * steps_of(key, shape, pieces, -0.22, 0.18)
    return jnp.clip(entries, -reach, reach).astype(held_as)


def setup_inputs(seed: int = 0) -> dict:
    splits = jax.random.split(jax.random.key(seed), 13)
    normed_input = draw_normed_input(jax.random.fold_in(splits[12], 71), 0)
    norm_gain = jnp.clip(1.0 + 0.1 * jax.random.normal(splits[1], (D,), jnp.float32), 0.5, 1.5)
    norm_scale = jnp.clip(jnp.exp(math.log(4.0) - 2.3025851 * jax.random.uniform(splits[2], (SEQUENCE_COUNT, SEQUENCE_TOKENS), jnp.float32) ** steps_of(splits[2], (SEQUENCE_COUNT, SEQUENCE_TOKENS), ((0, 8),), -0.2, 0.2)), 0.4, 4.0)
    out_grad = bell_draw(splits[3], (SEQUENCE_COUNT, SEQUENCE_TOKENS, D), 1.0, 6.0, ((0, 8), (2, 4)))
    router_weight = draw_router_weight(jax.random.fold_in(splits[12], 71), 0)
    routed_experts_keys = jax.random.split(jax.random.fold_in(splits[5], 1), SEQUENCE_COUNT * SEQUENCE_TOKENS // SEQUENCE_TOKENS)
    routed_experts_turns = jax.random.permutation(jax.random.fold_in(splits[5], 3), SEQUENCE_COUNT * SEQUENCE_TOKENS // SEQUENCE_TOKENS)
    routed_experts = jax.vmap(lambda own, number: shared_out(jax.random.fold_in(splits[5], 2), own, number, SEQUENCE_TOKENS, EXPERTS, TOPK, CAP, 2))(routed_experts_keys, routed_experts_turns).reshape((SEQUENCE_COUNT, SEQUENCE_TOKENS, TOPK))
    expert_grad = draw_expert_grad(jax.random.fold_in(splits[12], 71), 0)
    gate_grad = bell_draw(splits[7], (EXPERTS, SEQUENCE_COUNT, CAP), 8.0, 48.0, ((0, 8),))
    out_proj = bell_draw(splits[8], (QUERY_HEADS * HEAD_WIDTH, D), (QUERY_HEADS * HEAD_WIDTH) ** -0.5, 0.0625, ((0, 4),))
    query_states = draw_query_states(jax.random.fold_in(splits[12], 71), 0)
    rotated_keys = draw_rotated_keys(jax.random.fold_in(splits[12], 71), 0)
    value_tensor = bell_draw(splits[11], (SEQUENCE_COUNT, SEQUENCE_TOKENS, KEY_VALUE_HEADS * HEAD_WIDTH), 1.0, 6.0, ((0, 8),))
    return dict(normed_input=normed_input, norm_gain=norm_gain, norm_scale=norm_scale, out_grad=out_grad, router_weight=router_weight, routed_experts=routed_experts, expert_grad=expert_grad, gate_grad=gate_grad, out_proj=out_proj, query_states=query_states, rotated_keys=rotated_keys, value_tensor=value_tensor)


def reference(normed_input, norm_gain, norm_scale, out_grad, router_weight, routed_experts, expert_grad, gate_grad, out_proj, query_states, rotated_keys, value_tensor):
    highest = lax.Precision.HIGHEST
    expert_iota = lax.iota(jnp.int32, EXPERTS)
    weight_full = router_weight.astype(jnp.float32)
    group_width = QUERY_HEADS // KEY_VALUE_HEADS
    resident_heads = QUERY_HEADS // N_HEAD
    replica_count = N_HEAD // KEY_VALUE_HEADS

    def per_sequence(sequence_index):
        hidden_part = normed_input[sequence_index].astype(jnp.float32)
        expert_ids = routed_experts[sequence_index].astype(jnp.int32)
        slot_table = expert_grad[:, sequence_index].reshape(EXPERTS * CAP, D)
        gate_table = gate_grad[:, sequence_index].reshape(EXPERTS * CAP)
        scaled = hidden_part * norm_gain
        normed = scaled.astype(jnp.bfloat16)
        logits = jnp.dot(normed, router_weight, preferred_element_type=jnp.float32)
        picked = jnp.take_along_axis(logits, expert_ids, axis=1)
        gate_weights = jax.nn.softmax(picked, axis=-1)
        member = expert_ids[:, :, None] == expert_iota[None, None, :]
        per_token = lax.optimization_barrier(jnp.sum(member.astype(jnp.int32), axis=1, dtype=jnp.int32))
        before = jnp.cumsum(per_token, axis=0, dtype=jnp.int32) - per_token
        slot_index = lax.optimization_barrier(jnp.sum(jnp.where(member, before[:, None, :], 0), axis=-1, dtype=jnp.int32))
        flat_index = (expert_ids * CAP + slot_index).astype(jnp.int32)
        slot_rows = jnp.take(slot_table, flat_index, axis=0).astype(jnp.float32)
        slot_grads = jnp.take(gate_table, flat_index).astype(jnp.float32)
        gate_diff = gate_weights * (slot_grads - lax.optimization_barrier(jnp.sum(gate_weights * slot_grads, axis=-1, keepdims=True)))
        diff_full = jnp.einsum('lk,lke->le', gate_diff, member.astype(jnp.float32), precision=highest)
        grad_normed = jnp.einsum('lk,lkd->ld', gate_weights, slot_rows, precision=highest)
        grad_normed = grad_normed + jnp.dot(diff_full, weight_full.T, precision=highest)
        inner = lax.optimization_barrier(jnp.sum(scaled * grad_normed, axis=-1))
        grad_hidden = out_grad[sequence_index].astype(jnp.float32) + norm_scale[sequence_index][:, None] * (norm_gain * grad_normed - hidden_part * inner[:, None] / D)
        grad_hidden = grad_hidden.astype(jnp.bfloat16)
        context_grad = jnp.dot(grad_hidden, out_proj.T, preferred_element_type=jnp.float32).astype(jnp.bfloat16)
        queries = query_states[sequence_index].reshape(SEQUENCE_TOKENS, QUERY_HEADS, HEAD_WIDTH).astype(jnp.float32)
        key_row_block = jnp.repeat(rotated_keys[sequence_index].reshape(SEQUENCE_TOKENS, KEY_VALUE_HEADS, HEAD_WIDTH), group_width, axis=1).astype(jnp.float32)
        value_row_block = jnp.repeat(value_tensor[sequence_index].reshape(SEQUENCE_TOKENS, KEY_VALUE_HEADS, HEAD_WIDTH), group_width, axis=1).astype(jnp.float32)
        grads_ctx = context_grad.reshape(SEQUENCE_TOKENS, QUERY_HEADS, HEAD_WIDTH).astype(jnp.float32)
        root = jnp.sqrt(jnp.float32(HEAD_WIDTH))
        scores = jnp.einsum('qhd,khd->hqk', queries, key_row_block) / root
        positions = lax.iota(jnp.int32, SEQUENCE_TOKENS)
        causal = positions[:, None] >= positions[None, :]
        scores = jnp.where(causal[None], scores, -jnp.inf)
        attn_probs = jax.nn.softmax(scores, axis=-1)
        probs_low = attn_probs.astype(jnp.bfloat16)
        prob_grads = jnp.einsum('qhd,khd->hqk', grads_ctx, value_row_block)
        row_delta = lax.optimization_barrier(jnp.sum(attn_probs * prob_grads, axis=-1, keepdims=True))
        score_grads = (attn_probs * (prob_grads - row_delta) / root).astype(jnp.bfloat16)
        score_f = score_grads.astype(jnp.float32)
        grad_query = jnp.einsum('hqk,khd->qhd', score_f, key_row_block).astype(jnp.bfloat16).reshape(SEQUENCE_TOKENS, QUERY_HEADS * HEAD_WIDTH)
        key_heads = jnp.einsum('hqk,qhd->hkd', score_f, queries)
        value_heads = jnp.einsum('hqk,qhd->hkd', probs_low.astype(jnp.float32), grads_ctx)
        partial_key_sum = lax.optimization_barrier(jnp.sum(key_heads.reshape(N_HEAD, resident_heads, SEQUENCE_TOKENS, HEAD_WIDTH), axis=1)).astype(jnp.bfloat16)
        partial_value_sum = lax.optimization_barrier(jnp.sum(value_heads.reshape(N_HEAD, resident_heads, SEQUENCE_TOKENS, HEAD_WIDTH), axis=1)).astype(jnp.bfloat16)
        key_gradient = lax.optimization_barrier(jnp.sum(partial_key_sum.astype(jnp.float32).reshape(KEY_VALUE_HEADS, replica_count, SEQUENCE_TOKENS, HEAD_WIDTH), axis=1)).astype(jnp.bfloat16)
        value_gradient = lax.optimization_barrier(jnp.sum(partial_value_sum.astype(jnp.float32).reshape(KEY_VALUE_HEADS, replica_count, SEQUENCE_TOKENS, HEAD_WIDTH), axis=1)).astype(jnp.bfloat16)
        key_gradient = jnp.transpose(key_gradient, (1, 0, 2)).reshape(SEQUENCE_TOKENS, KEY_VALUE_HEADS * HEAD_WIDTH)
        value_gradient = jnp.transpose(value_gradient, (1, 0, 2)).reshape(SEQUENCE_TOKENS, KEY_VALUE_HEADS * HEAD_WIDTH)
        return (grad_hidden, grad_query, key_gradient, value_gradient)
    results = lax.map(per_sequence, jnp.arange(SEQUENCE_COUNT, dtype=jnp.int32))
    return (results[0], results[1], results[2], results[3])
```

```python
import functools
import math

import jax
import jax.numpy as jnp
from jax import lax
from jax.experimental import pallas as pl
from jax.experimental.pallas import tpu as pltpu
from jax.sharding import PartitionSpec as P

QUERY_HEADS = 64
KEY_VALUE_HEADS = 4
HEAD_WIDTH = 128
MESH = pl.DeviceIdType.MESH
NT = (((1,), (1,)), ((), ()))
TN = (((0,), (0,)), ((), ()))
F32 = jnp.float32
BF16 = jnp.bfloat16


def mm(a, b, dims=(((1,), (0,)), ((), ()))):
    return lax.dot_general(a, b, dims, preferred_element_type=F32)


def kernel(
    n_exp, n_head, width_total,
    x_hbm, gain_hbm, scale_hbm, og_hbm, router_hbm, ids_hbm, expert_hbm, gg_hbm, proj_ref,
    q_hbm, k_hbm, v_hbm,
    gh_out, gq_out, gk_out, gv_out,
    gain_ref, scale_ref, og_ref, router_ref, ids_ref, expert_ref, gg_ref,
    q_ref, k_ref, v_ref, in_sem,
    w_v, row_send, rows, gg_in, logit, gt, gates, p_out, p_in, sg_out, sg_in, diff_v, inner_v, gh_all, x_all,
    ctx, probs_v, q_send, q_in, kv_send, kv_in,
    w_sem, send_sem, xr, ggr, lr, gr, pr, sr, inr, hr, xar, qr, kvr, up_sem, down_sem,
):
    e = lax.axis_index("exp")
    h = lax.axis_index("head")
    x = lax.rem(e, 2)
    z = e // 2
    cols = n_exp // 2
    seq, width = x_all.shape[1:]
    experts_all = router_ref.shape[0]
    local, cap = expert_ref.shape[:2]
    room = rows.shape[2] // local
    pair = 2 * local
    heads = proj_ref.shape[0] // HEAD_WIDTH
    tok = seq // n_head
    half = width // 2
    partner = 2 * z + 1 - x
    ROWS, GG, LOGIT, GATE, PART, SLOT, GH, INNER, XALL, QS, KVS = range(11)

    def exp_peer(i):
        return {"exp": 2 * i + x}

    def send(src, dst, s_sem, r_sem, to):
        return pltpu.make_async_remote_copy(
            src_ref=src, dst_ref=dst, send_sem=send_sem.at[s_sem], recv_sem=r_sem,
            device_id=to, device_id_type=MESH,
        )

    def drain(ref, sem):
        pltpu.make_async_copy(ref, ref, sem).wait()

    chips = n_head // 2
    chip, core = h // 2, lax.rem(h, 2)
    sibling = 2 * chip + 1 - core
    same, cross = [], []
    for i in range(1, chips):
        there = 2 * lax.rem(chip + i, chips)
        same.append(there + core)
        cross.append(there + 1 - core)
    head_peers = [sibling] + same + cross
    if cols == 4:
        col_peers = [3 * (1 - z // 2), 2 - z // 2, z + 1 - 2 * lax.rem(z, 2)]
    else:
        col_peers = [lax.rem(z + i, cols) for i in range(1, cols)]
    all_cols = col_peers + [z]

    barrier = pltpu.get_barrier_semaphore()
    pl.semaphore_signal(barrier, inc=1, device_id={"exp": partner}, device_id_type=MESH)
    for p in head_peers:
        pl.semaphore_signal(barrier, inc=1, device_id={"head": p}, device_id_type=MESH)

    @pl.when(z > 0)
    def _():
        pl.semaphore_signal(barrier, inc=1, device_id=exp_peer(z - 1), device_id_type=MESH)

    @pl.when(z < cols - 1)
    def _():
        pl.semaphore_signal(barrier, inc=1, device_id=exp_peer(z + 1), device_id_type=MESH)

    greeted = 1 + (n_head - 1) + (z + cols - 1) // cols + (2 * cols - 2 - z) // cols

    loads = {}
    for i, (name, src, dst) in enumerate((
        ("x", x_hbm, x_all.at[h]), ("gain", gain_hbm, gain_ref), ("router", router_hbm, router_ref),
        ("expert", expert_hbm, expert_ref), ("gg", gg_hbm, gg_ref), ("ids", ids_hbm, ids_ref),
        ("q", q_hbm, q_ref), ("k", k_hbm, k_ref), ("v", v_hbm, v_ref), ("og", og_hbm, og_ref),
        ("scale", scale_hbm, scale_ref),
    )):
        loads[name] = pltpu.make_async_copy(src, dst, in_sem.at[i])
    for cp in loads.values():
        cp.start()
    w_copies = [
        pltpu.make_async_copy(proj_ref.at[:, pl.ds(j * width, width)], w_v.at[j], w_sem)
        for j in range(n_head)
    ]

    for name in ("x", "gain", "router"):
        loads[name].wait()
    gain = gain_ref[...]

    def hidden_f32():
        return x_all[h].astype(F32)

    logit[h] = mm(router_ref[...], (hidden_f32() * gain).astype(BF16), NT)
    pl.semaphore_wait(barrier, greeted)

    def logit_copy(src, to):
        return send(logit.at[src], logit.at[src], LOGIT, lr, {"head": to})

    def x_copy(src, to):
        return send(x_all.at[src], x_all.at[src], XALL, xar, {"head": to})

    for p in head_peers:
        logit_copy(h, p).start()

    if cols > 2:
        @pl.when(z == 1)
        def _():
            pl.semaphore_signal(up_sem, inc=1, device_id=exp_peer(z + 1), device_id_type=MESH)

        @pl.when(z == cols - 2)
        def _():
            pl.semaphore_signal(down_sem, inc=1, device_id=exp_peer(z - 1), device_id_type=MESH)

    for p in head_peers:
        x_copy(h, p).start()
    loads["gg"].wait()
    gg_copy = send(gg_ref, gg_in, GG, ggr, {"exp": partner})
    gg_copy.start()

    loads["expert"].wait()
    for cp in w_copies:
        cp.start()
    flat = expert_ref.reshape(local, cap * n_exp, width)

    def pick(c_list, side):
        m = len(c_list) * room
        r_i = lax.broadcasted_iota(jnp.int32, (m, cap * n_exp), 0)
        k_i = lax.broadcasted_iota(jnp.int32, (m, cap * n_exp), 1)
        group = r_i // room
        number = jnp.zeros_like(r_i)
        for i, c in enumerate(c_list):
            number = jnp.where(group == i, 2 * c + side, number)
        slot = r_i - group * room
        one = jnp.logical_and(slot < cap, slot * n_exp + number == k_i)
        return jnp.where(one, 1.0, 0.0).astype(BF16)

    def row_copy(c, j):
        part = pl.ds(j * room, room)
        return send(row_send.at[c, part], rows.at[c, x, part], ROWS, xr.at[c], {"exp": partner})

    step = min(cols, 4)
    for first in range(0, cols, step):
        some = all_cols[first : first + step]
        chosen = pick(some, 1 - x)
        for j in range(local):
            got = mm(chosen, flat[j]).astype(BF16)
            for i, c in enumerate(some):
                row_send[c, j * room : (j + 1) * room] = got[i * room : (i + 1) * room]
            row_copy(some[0], j).start()
        for c in some[1:]:
            for j in range(local):
                row_copy(c, j).start()

    for first in range(0, cols, step):
        some = all_cols[first : first + step]
        chosen = pick(some, x)
        for j in range(local):
            got = mm(chosen, flat[j]).astype(BF16)
            for i, c in enumerate(some):
                rows[c, x, j * room : (j + 1) * room] = got[i * room : (i + 1) * room]

    if cols > 3:
        @pl.when(jnp.logical_and(z > 1, z < cols - 1))
        def _():
            pl.semaphore_wait(up_sem, 1)
            pl.semaphore_signal(up_sem, inc=1, device_id=exp_peer(z + 1), device_id_type=MESH)

        @pl.when(jnp.logical_and(z > 0, z < cols - 2))
        def _():
            pl.semaphore_wait(down_sem, 1)
            pl.semaphore_signal(down_sem, inc=1, device_id=exp_peer(z - 1), device_id_type=MESH)

    for name in ("ids", "q", "k", "v"):
        loads[name].wait()
    kv = h * heads // (QUERY_HEADS // KEY_VALUE_HEADS)
    lanes = pl.ds(pl.multiple_of(kv * HEAD_WIDTH, HEAD_WIDTH), HEAD_WIDTH)

    def stacked(a):
        return jnp.concatenate(
            [a[:, i * HEAD_WIDTH : (i + 1) * HEAD_WIDTH] for i in range(a.shape[1] // HEAD_WIDTH)],
            axis=0,
        )

    inv_sqrt = 1.0 / math.sqrt(HEAD_WIDTH)
    scores = mm(stacked(q_ref[...]), k_ref[:, lanes], NT) * inv_sqrt
    position = lax.rem(lax.broadcasted_iota(jnp.int32, scores.shape, 0), seq)
    causal = position >= lax.broadcasted_iota(jnp.int32, scores.shape, 1)
    scores = jnp.where(causal, scores, -jnp.inf)
    probs = jnp.exp(scores - jnp.max(scores, axis=1, keepdims=True))
    probs_v[...] = probs / jnp.sum(probs, axis=1, keepdims=True)

    expert_i = lax.broadcasted_iota(jnp.int32, (experts_all, seq), 0)
    member = ids_ref[0:1] == expert_i
    for i in range(1, ids_ref.shape[0]):
        member = jnp.logical_or(member, ids_ref[i : i + 1] == expert_i)
    row_i = lax.broadcasted_iota(jnp.int32, (seq, seq), 0)
    col_i = lax.broadcasted_iota(jnp.int32, (seq, seq), 1)

    if n_head > 1:
        drain(logit.at[pl.ds(0, n_head - 1)], lr)
    total = logit[0]
    for i in range(1, n_head):
        total = total + logit[i]
    total = jnp.where(member, total, -jnp.inf)
    top = jnp.max(total, axis=0, keepdims=True)
    weights = jnp.exp(total - top)
    weights = weights / jnp.sum(weights, axis=0, keepdims=True)
    weights_t = jnp.where(member, weights, -1.0)
    for c in range(cols):
        gt[c] = weights_t[c * pair : (c + 1) * pair]

    def gate_copy(c):
        return send(gt.at[c], gates.at[z], GATE, gr.at[z], exp_peer(c))

    def gate_wait(c):
        return send(gt.at[c], gates.at[c], GATE, gr.at[c], exp_peer(c))

    def far():
        if cols > 2:
            @pl.when(z == 0)
            def _():
                pl.semaphore_wait(down_sem, 1)

            @pl.when(z == cols - 1)
            def _():
                pl.semaphore_wait(up_sem, 1)

    if cols != 4:
        far()
    for i, c in enumerate(reversed(col_peers)):
        gate_copy(c).start()
        if cols == 4 and i == 0:
            far()

    earlier = (row_i < col_i).astype(BF16)
    slot_i = lax.broadcasted_iota(jnp.int32, (room, seq), 0)
    seq_i = lax.broadcasted_iota(jnp.int32, (n_exp, seq), 0)
    gg_copy.wait_recv()

    def contribution(c, w):
        named = w >= 0.0
        before = mm(jnp.where(named, 1.0, 0.0).astype(BF16), earlier).astype(jnp.int32)
        slot_grads = []
        spread = []
        for j in range(pair):
            hit = jnp.logical_and(before[j : j + 1] == slot_i, named[j : j + 1])
            spread.append(jnp.where(hit, w[j : j + 1], 0.0).astype(BF16))
            own_g = gg_ref[j % local].astype(F32)
            far_g = gg_in[j % local].astype(F32)
            table = jnp.where(x == j // local, own_g, far_g).astype(BF16)
            by_seq = mm(table, jnp.where(hit[:cap], 1.0, 0.0).astype(BF16))
            slot_grads.append(
                jnp.sum(jnp.where(seq_i == 2 * c + x, by_seq, 0.0), axis=0, keepdims=True)
            )
        return jnp.concatenate(spread, axis=0), slot_grads

    def weigh(c, spread):
        return mm(spread, rows[c].reshape(pair * room, width), TN)

    def row_wait(c):
        drain(rows.at[c, 1 - x], xr.at[c])

    def part_copy(c):
        return send(p_out.at[c], p_in.at[z], PART, pr.at[z], exp_peer(c))

    def slot_copy(c):
        return send(sg_out.at[c], sg_in.at[z], SLOT, sr, exp_peer(c))

    spread_z, slot_grads = contribution(z, gt[z])
    for j in range(pair):
        sg_in[z, j : j + 1] = slot_grads[j]
    for i, c in enumerate(col_peers):
        gate_wait(c).wait_recv()
        spread, slot_grads = contribution(c, gates[c])
        for j in range(pair):
            sg_out[c, j : j + 1] = slot_grads[j]
        slot_copy(c).start()
        row_wait(c)
        p_out[c] = weigh(c, spread).astype(BF16)
        part_copy(c).start()
    if cols > 1:
        drain(sg_in.at[pl.ds(0, cols - 1)], sr)
    mean = jnp.zeros((1, seq), F32)
    for c in range(cols):
        mean = mean + jnp.sum(jnp.maximum(gt[c], 0.0) * sg_in[c], axis=0, keepdims=True)
    for c in range(cols):
        diff_v[c * pair : (c + 1) * pair] = jnp.maximum(gt[c], 0.0) * (sg_in[c] - mean)
    diff = diff_v[...]
    diff_hi = diff.astype(BF16)
    diff_lo = (diff - diff_hi.astype(F32)).astype(BF16)
    grad = mm(diff_hi, router_ref[...], TN) + mm(diff_lo, router_ref[...], TN)
    loads["og"].wait()
    loads["scale"].wait()
    scale = jnp.sum(
        jnp.where(row_i == col_i, jnp.broadcast_to(scale_ref[...], (seq, seq)), 0.0),
        axis=1, keepdims=True,
    )
    row_wait(z)
    grad = grad + weigh(z, spread_z)
    for i, c in enumerate(col_peers):
        drain(p_in.at[c], pr.at[c])
        grad = grad + p_in[c].astype(F32)


    def gh_copy(src, k, to):
        return send(
            gh_all.at[src, k], gh_all.at[src, k], GH, hr.at[src, k], {"head": to}
        )

    def half_of(a, k):
        return a[:, k * half : (k + 1) * half]

    base = []
    for k in range(2):
        base.append(
            half_of(og_ref[...], k).astype(F32) + scale * (half_of(gain, k) * half_of(grad, k))
        )
        gh_all[h, k] = base[k].astype(BF16)
        for p in [sibling] + same:
            gh_copy(h, k, p).start()
    for p in cross:
        for k in range(2):
            gh_copy(h, k, p).start()
    inner_v[h] = jnp.broadcast_to(
        jnp.sum(hidden_f32() * gain * grad, axis=1, keepdims=True), (seq, HEAD_WIDTH)
    )

    def inner_copy(src, to):
        return send(inner_v.at[src], inner_v.at[src], INNER, inr, {"head": to})

    for p in head_peers:
        inner_copy(h, p).start()
    drain(w_v, w_sem)
    if n_head > 1:
        drain(x_all.at[pl.ds(0, n_head - 1)], xar)

    rows_w = w_v.shape[1]
    tile = min(512, rows_w)
    per = tile // HEAD_WIDTH

    def piece(p, k):
        return (
            jnp.concatenate([gh_all[p, k], x_all[p, :, k * half : (k + 1) * half]], axis=0),
            k * half, half,
        )

    def whole(p):
        return (
            jnp.concatenate(
                [jnp.concatenate([gh_all[p, 0], gh_all[p, 1]], axis=1), x_all[p]], axis=0
            ),
            0, width,
        )

    def product(p, block, r):
        a, at, size = block
        return mm(a, w_v[p, r : r + tile, at : at + size], NT)

    stages = [(h, None)] + [(sibling, None)]
    for p in same + cross:
        stages += [(p, 0), (p, 1)]
    for i, (p, k) in enumerate(stages[:-1]):
        if i:
            for kk in (0, 1) if k is None else (k,):
                drain(gh_all.at[p, kk], hr.at[p, kk])
        block = whole(p) if k is None else piece(p, k)
        for r in range(0, rows_w, tile):
            part = product(p, block, r)
            if i:
                part = ctx[:, r : r + tile] + part
            ctx[:, r : r + tile] = part

    if n_head > 1:
        drain(inner_v.at[pl.ds(0, n_head - 1)], inr)
    inner = inner_v[0]
    for i in range(1, n_head):
        inner = inner + inner_v[i]
    taken = scale * inner[:, 0:1] / width_total

    p, k = stages[-1]
    if k is None:
        for kk in (0, 1):
            drain(gh_all.at[p, kk], hr.at[p, kk])
        block = whole(p)
    else:
        drain(gh_all.at[p, k], hr.at[p, k])
        block = piece(p, k)
    key_block = k_ref[:, lanes]
    value_block = v_ref[:, lanes]
    gk = jnp.zeros((seq, HEAD_WIDTH), F32)
    gv = jnp.zeros((seq, HEAD_WIDTH), F32)

    def q_copy(r, to):
        at = pl.ds(r, tile)
        return send(q_send.at[to, :, at], q_in.at[h, :, at], QS, qr, {"head": to})

    def kv_copy(to):
        return send(kv_send.at[to], kv_in.at[h], KVS, kvr, {"head": to})

    for r in range(0, rows_w, tile):
        part = ctx[:, r : r + tile] + product(p, block, r)
        ctx_s = stacked((part[:seq] - taken * part[seq:]).astype(BF16))
        first = r // HEAD_WIDTH
        probs = probs_v[first * seq : (first + per) * seq]
        prob_grads = mm(ctx_s, value_block, NT)
        delta = jnp.sum(probs * prob_grads, axis=1, keepdims=True)
        score_grads = (probs * (prob_grads - delta) * inv_sqrt).astype(BF16)
        gq = mm(score_grads, key_block).astype(BF16)
        for d in range(n_head):
            for i in range(per):
                s = i * seq + d * tok
                q_send[d, :, r + i * HEAD_WIDTH : r + (i + 1) * HEAD_WIDTH] = gq[s : s + tok]
        for to in head_peers:
            q_copy(r, to).start()
        gk = gk + mm(score_grads, stacked(q_ref[:, r : r + tile]), TN)
        gv = gv + mm(probs.astype(BF16), ctx_s, TN)
    for d in range(n_head):
        kv_send[d, 0] = gk[d * tok : (d + 1) * tok].astype(BF16)
        kv_send[d, 1] = gv[d * tok : (d + 1) * tok].astype(BF16)
    for to in head_peers:
        kv_copy(to).start()
    for k in range(2):
        gh_out[:, k * half : (k + 1) * half] = (
            base[k] - half_of(hidden_f32(), k) * taken
        ).astype(BF16)
    q_in[h] = q_send[h]
    kv_in[h] = kv_send[h]

    others = pl.ds(0, n_head - 1)
    some_cols = pl.ds(0, cols - 1)
    sent = [(row_send, ROWS)]
    if cols > 1:
        sent += [(gt.at[some_cols], GATE), (p_out.at[some_cols], PART), (sg_out.at[some_cols], SLOT)]
    if n_head > 1:
        sent += [
            (logit.at[others], LOGIT), (x_all.at[others], XALL), (gh_all.at[others], GH),
            (inner_v.at[others], INNER),
        ]
    gg_copy.wait_send()
    for ref, which in sent:
        drain(ref, send_sem.at[which])
    if n_head > 1:
        drain(q_in.at[others], qr)
        drain(kv_in.at[others], kvr)
    span = heads * HEAD_WIDTH
    for i in range(n_head):
        gq_out[:, i * span : (i + 1) * span] = q_in[i]
    replicas = n_head // KEY_VALUE_HEADS
    for g in range(KEY_VALUE_HEADS):
        for k, out in enumerate((gk_out, gv_out)):
            total = kv_in[g * replicas, k].astype(F32)
            for i in range(1, replicas):
                total = total + kv_in[g * replicas + i, k].astype(F32)
            out[:, g * HEAD_WIDTH : (g + 1) * HEAD_WIDTH] = total.astype(BF16)
    if n_head > 1:
        drain(q_send.at[others], send_sem.at[QS])
        drain(kv_send.at[others], send_sem.at[KVS])


def write_out(*refs):
    n = (len(refs) - 1) // 2
    sems = refs[-1]
    copies = [
        pltpu.make_async_copy(refs[i], refs[n + i], sems.at[i]) for i in range(n)
    ]
    for cp in copies:
        cp.start()
    for cp in copies:
        cp.wait()


def solution(mesh):
    n_exp = mesh.shape["exp"]
    n_head = mesh.shape["head"]
    cols = n_exp // 2

    def per_device(
        normed_input, norm_gain, norm_scale, out_grad, router_weight, routed_experts,
        expert_grad, gate_grad, out_proj, query_states, rotated_keys, value_tensor,
    ):
        _, seq, width = normed_input.shape
        experts_all = router_weight.shape[1]
        local, _, cap, _ = expert_grad.shape
        pair = 2 * local
        span, width_total = out_proj.shape
        heads = span // HEAD_WIDTH
        tok = seq // n_head
        kv_width = rotated_keys.shape[2]
        vm = pltpu.VMEM
        dma = pltpu.SemaphoreType.DMA
        vmem = pl.BlockSpec(memory_space=pltpu.VMEM)
        hbm = pl.BlockSpec(memory_space=pltpu.HBM)
        room = -(-cap // 16) * 16
        top_k = routed_experts.shape[2]
        outs = pl.pallas_call(
            functools.partial(kernel, n_exp, n_head, width_total),
            name="moe_attention_backward",
            out_shape=(
                jax.ShapeDtypeStruct((seq, width), BF16),
                jax.ShapeDtypeStruct((tok, n_head * span), BF16),
                jax.ShapeDtypeStruct((tok, kv_width), BF16),
                jax.ShapeDtypeStruct((tok, kv_width), BF16),
            ),
            in_specs=[hbm] * 12,
            out_specs=(vmem,) * 4,
            scratch_shapes=[
                vm((1, width), F32), vm((1, seq), F32),
                vm((seq, width), BF16), vm((experts_all, width), BF16),
                vm((top_k, seq), jnp.int32), vm((local, cap, n_exp, width), BF16),
                vm(gate_grad.shape, BF16), vm((seq, span), BF16),
                vm((seq, kv_width), BF16), vm((seq, kv_width), BF16), dma((11,)),
                vm((n_head, span, width), BF16),
                vm((cols, local * room, width), BF16),
                vm((cols, 2, local * room, width), BF16),
                vm(gate_grad.shape, BF16),
                vm((n_head, experts_all, seq), F32),
                vm((cols, pair, seq), F32),
                vm((cols, pair, seq), F32),
                vm((cols, seq, width), BF16),
                vm((cols, seq, width), BF16),
                vm((cols, pair, seq), F32),
                vm((cols, pair, seq), F32),
                vm((experts_all, seq), F32),
                vm((n_head, seq, HEAD_WIDTH), F32),
                vm((n_head, 2, seq, width // 2), BF16),
                vm((n_head, seq, width), BF16),
                vm((2 * seq, span), F32),
                vm((heads * seq, seq), F32),
                vm((n_head, tok, span), BF16),
                vm((n_head, tok, span), BF16),
                vm((n_head, 2, tok, HEAD_WIDTH), BF16),
                vm((n_head, 2, tok, HEAD_WIDTH), BF16),
                dma, dma((11,)), dma((cols,)), dma, dma, dma((cols,)), dma((cols,)), dma,
                dma, dma((n_head, 2)), dma, dma, dma,
                pltpu.SemaphoreType.REGULAR, pltpu.SemaphoreType.REGULAR,
            ],
            compiler_params=pltpu.CompilerParams(
                collective_id=0, has_side_effects=True, vmem_limit_bytes=48 * 1024 * 1024
            ),
        )(
            *(
                pltpu.with_memory_space_constraint(a, pltpu.HBM)
                for a in (
                    normed_input[0], norm_gain[None], norm_scale, out_grad[0], router_weight.T,
                    routed_experts[0].T, jnp.transpose(expert_grad, (0, 2, 1, 3)), gate_grad,
                    out_proj, query_states[0], rotated_keys[0], value_tensor[0],
                )
            )
        )
        outs = pl.pallas_call(
            write_out,
            name="write_out",
            out_shape=tuple(jax.ShapeDtypeStruct(o.shape, o.dtype) for o in outs),
            in_specs=[vmem] * 4,
            out_specs=(hbm,) * 4,
            scratch_shapes=[dma((4,))],
            compiler_params=pltpu.CompilerParams(vmem_limit_bytes=1024 * 1024),
        )(*outs)
        return tuple(o[None] for o in outs)

    placed = (
        P("exp", None, "head"),
        P("head"),
        P("exp", None),
        P("exp", None, "head"),
        P("head", None),
        P("exp", None, None),
        P("exp", None, None, "head"),
        P("exp", None, None),
        P("head", None),
        P("exp", None, "head"),
        P("exp", None, None),
        P("exp", None, None),
    )
    return jax.shard_map(
        per_device,
        mesh=mesh,
        in_specs=placed,
        out_specs=(
            P("exp", None, "head"),
            P("exp", "head", None),
            P("exp", "head", None),
            P("exp", "head", None),
        ),
        check_vma=False,
    )
```

```python
import functools
import math

import jax
import jax.numpy as jnp
from jax import lax
from jax.experimental import pallas as pl
from jax.experimental.pallas import tpu as pltpu
from jax.sharding import PartitionSpec as P

QUERY_HEADS = 64
KEY_VALUE_HEADS = 4
HEAD_WIDTH = 128
MESH = pl.DeviceIdType.MESH
NT = (((1,), (1,)), ((), ()))
TN = (((0,), (0,)), ((), ()))
F32 = jnp.float32
BF16 = jnp.bfloat16


def mm(a, b, dims=(((1,), (0,)), ((), ()))):
    return lax.dot_general(a, b, dims, preferred_element_type=F32)


def kernel(
    n_exp, n_head, width_total,
    x_hbm, gain_hbm, scale_hbm, og_hbm, router_hbm, ids_hbm, expert_hbm, gg_hbm, proj_ref,
    q_hbm, k_hbm, v_hbm,
    gh_out, gq_out, gk_out, gv_out,
    gain_ref, scale_ref, og_ref, router_ref, ids_ref, expert_ref, gg_ref,
    q_ref, k_ref, v_ref, in_sem,
    w_v, row_send, rows, gg_in, logit, gt, gates, p_out, p_in, sg_out, sg_in, diff_v, inner_v, gh_all, x_all,
    ctx, probs_v, q_send, q_in, kv_send, kv_in, across, across_out, s_out, s_in,
    w_sem, send_sem, xr, ggr, lr, gr, pr, sr, inr, hr, xar, qr, kvr, acr, shr, up_sem, down_sem,
):
    e = lax.axis_index("exp")
    h = lax.axis_index("head")
    x = lax.rem(e, 2)
    z = e // 2
    cols = n_exp // 2
    seq, width = x_all.shape[1:]
    experts_all = router_ref.shape[0]
    local, cap = expert_ref.shape[:2]
    room = rows.shape[2] // local
    pair = 2 * local
    heads = proj_ref.shape[0] // HEAD_WIDTH
    tok = seq // n_head
    half = width // 2
    partner = 2 * z + 1 - x
    ROWS, GG, LOGIT, GATE, PART, SLOT, GH, INNER, XALL, QS, KVS, ACROSS, SHARE = range(13)

    def exp_peer(i):
        return {"exp": 2 * i + x}

    def send(src, dst, s_sem, r_sem, to):
        return pltpu.make_async_remote_copy(
            src_ref=src, dst_ref=dst, send_sem=send_sem.at[s_sem], recv_sem=r_sem,
            device_id=to, device_id_type=MESH,
        )

    def drain(ref, sem):
        pltpu.make_async_copy(ref, ref, sem).wait()

    chips = n_head // 2
    chip, core = h // 2, lax.rem(h, 2)
    sibling = 2 * chip + 1 - core
    same, cross = [], []
    for i in range(1, chips):
        there = 2 * lax.rem(chip + i, chips)
        same.append(there + core)
        cross.append(there + 1 - core)
    head_peers = [sibling] + same + cross
    col_peers = [i + (i + cols - z) // cols for i in range(cols - 1)]
    all_cols = col_peers + [z]

    barrier = pltpu.get_barrier_semaphore()
    pl.semaphore_signal(barrier, inc=1, device_id={"exp": partner}, device_id_type=MESH)
    for p in head_peers:
        pl.semaphore_signal(barrier, inc=1, device_id={"head": p}, device_id_type=MESH)

    @pl.when(z > 0)
    def _():
        pl.semaphore_signal(barrier, inc=1, device_id=exp_peer(z - 1), device_id_type=MESH)

    @pl.when(z < cols - 1)
    def _():
        pl.semaphore_signal(barrier, inc=1, device_id=exp_peer(z + 1), device_id_type=MESH)

    greeted = 1 + (n_head - 1) + (z + cols - 1) // cols + (2 * cols - 2 - z) // cols

    loads = {}
    for i, (name, src, dst) in enumerate((
        ("x", x_hbm, x_all.at[h]), ("gain", gain_hbm, gain_ref), ("router", router_hbm, router_ref),
        ("expert", expert_hbm, expert_ref), ("gg", gg_hbm, gg_ref), ("ids", ids_hbm, ids_ref),
        ("q", q_hbm, q_ref), ("k", k_hbm, k_ref), ("v", v_hbm, v_ref), ("og", og_hbm, og_ref),
        ("scale", scale_hbm, scale_ref),
    )):
        loads[name] = pltpu.make_async_copy(src, dst, in_sem.at[i])
    for cp in loads.values():
        cp.start()
    w_copies = [
        pltpu.make_async_copy(proj_ref.at[:, pl.ds(j * width, width)], w_v.at[j], w_sem)
        for j in range(n_head)
    ]

    for name in ("x", "gain", "router"):
        loads[name].wait()
    gain = gain_ref[...]

    def hidden_f32():
        return x_all[h].astype(F32)

    logit[h] = mm(router_ref[...], (hidden_f32() * gain).astype(BF16), NT)
    pl.semaphore_wait(barrier, greeted)

    def logit_copy(src, to):
        return send(logit.at[src], logit.at[src], LOGIT, lr, {"head": to})

    def x_copy(src, to):
        return send(x_all.at[src], x_all.at[src], XALL, xar, {"head": to})

    for p in head_peers:
        logit_copy(h, p).start()

    if cols > 2:
        @pl.when(z == 1)
        def _():
            pl.semaphore_signal(up_sem, inc=1, device_id=exp_peer(z + 1), device_id_type=MESH)

        @pl.when(z == cols - 2)
        def _():
            pl.semaphore_signal(down_sem, inc=1, device_id=exp_peer(z - 1), device_id_type=MESH)

    for p in head_peers:
        x_copy(h, p).start()
    loads["gg"].wait()
    gg_copy = send(gg_ref, gg_in, GG, ggr, {"exp": partner})
    gg_copy.start()

    loads["expert"].wait()
    for cp in w_copies:
        cp.start()
    flat = expert_ref.reshape(local, cap * n_exp, width)

    def pick(c_list, side):
        m = len(c_list) * room
        r_i = lax.broadcasted_iota(jnp.int32, (m, cap * n_exp), 0)
        k_i = lax.broadcasted_iota(jnp.int32, (m, cap * n_exp), 1)
        group = r_i // room
        number = jnp.zeros_like(r_i)
        for i, c in enumerate(c_list):
            number = jnp.where(group == i, 2 * c + side, number)
        slot = r_i - group * room
        one = jnp.logical_and(slot < cap, slot * n_exp + number == k_i)
        return jnp.where(one, 1.0, 0.0).astype(BF16)

    def row_copy(c, j):
        part = pl.ds(j * room, room)
        return send(row_send.at[c, part], rows.at[c, 1, part], ROWS, xr.at[c], {"exp": partner})

    row_order = [(c, j) for c in col_peers for j in range(local)]
    held = len(row_order) // 2
    step = min(cols, 4)
    for first in range(0, cols, step):
        some = all_cols[first : first + step]
        chosen = pick(some, 1 - x)
        for j in range(local):
            got = mm(chosen, flat[j]).astype(BF16)
            for i, c in enumerate(some):
                row_send[c, j * room : (j + 1) * room] = got[i * room : (i + 1) * room]
            if cols > 1 and not first:
                row_copy(*row_order[j]).start()
    for c, j in row_order[local:held]:
        row_copy(c, j).start()

    for first in range(0, cols, step):
        some = all_cols[first : first + step]
        chosen = pick(some, x)
        for j in range(local):
            got = mm(chosen, flat[j]).astype(BF16)
            for i, c in enumerate(some):
                rows[c, 0, j * room : (j + 1) * room] = got[i * room : (i + 1) * room]

    if cols > 3:
        @pl.when(jnp.logical_and(z > 1, z < cols - 1))
        def _():
            pl.semaphore_wait(up_sem, 1)
            pl.semaphore_signal(up_sem, inc=1, device_id=exp_peer(z + 1), device_id_type=MESH)

        @pl.when(jnp.logical_and(z > 0, z < cols - 2))
        def _():
            pl.semaphore_wait(down_sem, 1)
            pl.semaphore_signal(down_sem, inc=1, device_id=exp_peer(z - 1), device_id_type=MESH)

    for name in ("ids", "q", "k", "v"):
        loads[name].wait()
    kv = h * heads // (QUERY_HEADS // KEY_VALUE_HEADS)
    lanes = pl.ds(pl.multiple_of(kv * HEAD_WIDTH, HEAD_WIDTH), HEAD_WIDTH)

    def stacked(a):
        return jnp.concatenate(
            [a[:, i * HEAD_WIDTH : (i + 1) * HEAD_WIDTH] for i in range(a.shape[1] // HEAD_WIDTH)],
            axis=0,
        )

    inv_sqrt = 1.0 / math.sqrt(HEAD_WIDTH)
    scores = mm(stacked(q_ref[...]), k_ref[:, lanes], NT) * inv_sqrt
    position = lax.rem(lax.broadcasted_iota(jnp.int32, scores.shape, 0), seq)
    causal = position >= lax.broadcasted_iota(jnp.int32, scores.shape, 1)
    scores = jnp.where(causal, scores, -jnp.inf)
    probs = jnp.exp(scores - jnp.max(scores, axis=1, keepdims=True))
    probs_v[...] = probs / jnp.sum(probs, axis=1, keepdims=True)

    expert_i = lax.broadcasted_iota(jnp.int32, (experts_all, seq), 0)
    member = ids_ref[0:1] == expert_i
    for i in range(1, ids_ref.shape[0]):
        member = jnp.logical_or(member, ids_ref[i : i + 1] == expert_i)
    row_i = lax.broadcasted_iota(jnp.int32, (seq, seq), 0)
    col_i = lax.broadcasted_iota(jnp.int32, (seq, seq), 1)

    if n_head > 1:
        drain(logit.at[pl.ds(0, n_head - 1)], lr)
    total = logit[0]
    for i in range(1, n_head):
        total = total + logit[i]
    total = jnp.where(member, total, -jnp.inf)
    top = jnp.max(total, axis=0, keepdims=True)
    weights = jnp.exp(total - top)
    weights = weights / jnp.sum(weights, axis=0, keepdims=True)
    weights_t = jnp.where(member, weights, -1.0)
    for c in range(cols):
        gt[c] = weights_t[c * pair : (c + 1) * pair]

    def gate_copy(c):
        return send(gt.at[c], gates.at[z], GATE, gr.at[z], exp_peer(c))

    def gate_wait(c):
        return send(gt.at[c], gates.at[c], GATE, gr.at[c], exp_peer(c))

    def by_side(a):
        low, high = a[:local], a[local:]
        return jnp.where(x == 0, low, high), jnp.where(x == 0, high, low)

    def far():
        if cols > 2:
            @pl.when(z == 0)
            def _():
                pl.semaphore_wait(down_sem, 1)

            @pl.when(z == cols - 1)
            def _():
                pl.semaphore_wait(up_sem, 1)

    across_out[...] = by_side(gt[z])[1]
    across_copy = send(across_out, across, ACROSS, acr, {"exp": partner})
    across_copy.start()
    for c, j in row_order[held:]:
        row_copy(c, j).start()
    far()
    for c in col_peers:
        gate_copy(c).start()

    earlier = (row_i < col_i).astype(BF16)
    slot_i = lax.broadcasted_iota(jnp.int32, (room, seq), 0)
    seq_i = lax.broadcasted_iota(jnp.int32, (n_exp, seq), 0)
    gg_copy.wait_recv()

    def places(w):
        named = w >= 0.0
        before = mm(jnp.where(named, 1.0, 0.0).astype(BF16), earlier).astype(jnp.int32)
        hits = []
        for j in range(w.shape[0]):
            hits.append(jnp.logical_and(before[j : j + 1] == slot_i, named[j : j + 1]))
        spread = [jnp.where(hit, w[j : j + 1], 0.0).astype(BF16) for j, hit in enumerate(hits)]
        return spread, hits

    def contribution(c, w, into):
        spread, hits = places(jnp.concatenate(by_side(w), axis=0))
        slots = []
        for j in range(pair):
            table = (gg_ref if j < local else gg_in)[j % local]
            by_seq = mm(table, jnp.where(hits[j][:cap], 1.0, 0.0).astype(BF16))
            slots.append(
                jnp.sum(jnp.where(seq_i == 2 * c + x, by_seq, 0.0), axis=0, keepdims=True)
            )
        for j in range(pair):
            into[c, j : j + 1] = jnp.where(x == 0, slots[j], slots[(j + local) % pair])
        return jnp.concatenate(spread, axis=0)

    def row_wait(c):
        drain(rows.at[c, 1], xr.at[c])

    s_copy = send(s_out, s_in, SHARE, shr, {"exp": partner})

    def share():
        across_copy.wait_recv()
        s_out[...] = mm(
            jnp.concatenate(places(across[...])[0], axis=0), row_send[z], TN
        ).astype(BF16)
        s_copy.start()

    def part_copy(c):
        return send(p_out.at[c], p_in.at[z], PART, pr.at[z], exp_peer(c))

    def slot_copy(c):
        return send(sg_out.at[c], sg_in.at[z], SLOT, sr, exp_peer(c))

    spread_z = contribution(z, gt[z], sg_in)
    grad = mm(spread_z[: local * room], rows[z, 0], TN)
    for i, c in enumerate(col_peers):
        gate_wait(c).wait_recv()
        spread = contribution(c, gates[c], sg_out)
        slot_copy(c).start()
        row_wait(c)
        p_out[c] = mm(spread, rows[c].reshape(pair * room, width), TN).astype(BF16)
        part_copy(c).start()
        if i == 0:
            share()
    if cols == 1:
        share()
    if cols > 1:
        drain(sg_in.at[pl.ds(0, cols - 1)], sr)
    mean = jnp.zeros((1, seq), F32)
    for c in range(cols):
        mean = mean + jnp.sum(jnp.maximum(gt[c], 0.0) * sg_in[c], axis=0, keepdims=True)
    for c in range(cols):
        diff_v[c * pair : (c + 1) * pair] = jnp.maximum(gt[c], 0.0) * (sg_in[c] - mean)
    diff = diff_v[...]
    diff_hi = diff.astype(BF16)
    diff_lo = (diff - diff_hi.astype(F32)).astype(BF16)
    grad = grad + mm(diff_hi, router_ref[...], TN) + mm(diff_lo, router_ref[...], TN)
    loads["og"].wait()
    loads["scale"].wait()
    scale = jnp.sum(
        jnp.where(row_i == col_i, jnp.broadcast_to(scale_ref[...], (seq, seq)), 0.0),
        axis=1, keepdims=True,
    )
    s_copy.wait_recv()
    grad = grad + s_in[...].astype(F32)
    for i, c in enumerate(col_peers):
        drain(p_in.at[c], pr.at[c])
        grad = grad + p_in[c].astype(F32)


    def gh_copy(src, k, to):
        return send(
            gh_all.at[src, k], gh_all.at[src, k], GH, hr.at[src, k], {"head": to}
        )

    def half_of(a, k):
        return a[:, k * half : (k + 1) * half]

    base = []
    for k in range(2):
        base.append(
            half_of(og_ref[...], k).astype(F32) + scale * (half_of(gain, k) * half_of(grad, k))
        )
        gh_all[h, k] = base[k].astype(BF16)
        for p in [sibling] + same:
            gh_copy(h, k, p).start()
    for p in cross:
        for k in range(2):
            gh_copy(h, k, p).start()
    inner_v[h] = jnp.broadcast_to(
        jnp.sum(hidden_f32() * gain * grad, axis=1, keepdims=True), (seq, HEAD_WIDTH)
    )

    def inner_copy(src, to):
        return send(inner_v.at[src], inner_v.at[src], INNER, inr, {"head": to})

    for p in head_peers:
        inner_copy(h, p).start()
    drain(w_v, w_sem)
    if n_head > 1:
        drain(x_all.at[pl.ds(0, n_head - 1)], xar)

    rows_w = w_v.shape[1]
    tile = min(512, rows_w)
    group = max(rows_w // 2, HEAD_WIDTH)
    per = group // HEAD_WIDTH

    def piece(p, k):
        return (
            jnp.concatenate([gh_all[p, k], x_all[p, :, k * half : (k + 1) * half]], axis=0),
            k * half, half,
        )

    def whole(p):
        return (
            jnp.concatenate(
                [jnp.concatenate([gh_all[p, 0], gh_all[p, 1]], axis=1), x_all[p]], axis=0
            ),
            0, width,
        )

    def product(p, block, r):
        a, at, size = block
        return mm(a, w_v[p, r : r + tile, at : at + size], NT)

    stages = [(h, None)] + [(sibling, None)]
    for p in same + cross:
        stages += [(p, 0), (p, 1)]
    for i, (p, k) in enumerate(stages[:-1]):
        if i:
            for kk in (0, 1) if k is None else (k,):
                drain(gh_all.at[p, kk], hr.at[p, kk])
        block = whole(p) if k is None else piece(p, k)
        for r in range(0, rows_w, tile):
            part = product(p, block, r)
            if i:
                part = ctx[:, r : r + tile] + part
            ctx[:, r : r + tile] = part

    if n_head > 1:
        drain(inner_v.at[pl.ds(0, n_head - 1)], inr)
    inner = inner_v[0]
    for i in range(1, n_head):
        inner = inner + inner_v[i]
    taken = scale * inner[:, 0:1] / width_total

    p, k = stages[-1]
    if k is None:
        for kk in (0, 1):
            drain(gh_all.at[p, kk], hr.at[p, kk])
        block = whole(p)
    else:
        drain(gh_all.at[p, k], hr.at[p, k])
        block = piece(p, k)
    key_block = k_ref[:, lanes]
    value_block = v_ref[:, lanes]
    gk = jnp.zeros((seq, HEAD_WIDTH), F32)
    gv = jnp.zeros((seq, HEAD_WIDTH), F32)

    def q_copy(r, to):
        at = pl.ds(r, group)
        return send(q_send.at[to, :, at], q_in.at[h, :, at], QS, qr, {"head": to})

    def kv_copy(to):
        return send(kv_send.at[to], kv_in.at[h], KVS, kvr, {"head": to})

    for r in range(0, rows_w, tile):
        ctx[:, r : r + tile] = ctx[:, r : r + tile] + product(p, block, r)
    for r in range(0, rows_w, group):
        part = ctx[:, r : r + group]
        ctx_s = stacked((part[:seq] - taken * part[seq:]).astype(BF16))
        first = r // HEAD_WIDTH
        probs = probs_v[first * seq : (first + per) * seq]
        prob_grads = mm(ctx_s, value_block, NT)
        delta = jnp.sum(probs * prob_grads, axis=1, keepdims=True)
        score_grads = (probs * (prob_grads - delta) * inv_sqrt).astype(BF16)
        gq = mm(score_grads, key_block).astype(BF16)
        for d in range(n_head):
            for i in range(per):
                s = i * seq + d * tok
                q_send[d, :, r + i * HEAD_WIDTH : r + (i + 1) * HEAD_WIDTH] = gq[s : s + tok]
        for to in head_peers:
            q_copy(r, to).start()
        gk = gk + mm(score_grads, stacked(q_ref[:, r : r + group]), TN)
        gv = gv + mm(probs.astype(BF16), ctx_s, TN)
    for d in range(n_head):
        kv_send[d, 0] = gk[d * tok : (d + 1) * tok].astype(BF16)
        kv_send[d, 1] = gv[d * tok : (d + 1) * tok].astype(BF16)
    for to in head_peers:
        kv_copy(to).start()
    for k in range(2):
        gh_out[:, k * half : (k + 1) * half] = (
            base[k] - half_of(hidden_f32(), k) * taken
        ).astype(BF16)
    q_in[h] = q_send[h]
    kv_in[h] = kv_send[h]

    others = pl.ds(0, n_head - 1)
    some_cols = pl.ds(0, cols - 1)
    sent = []
    if cols > 1:
        sent += [
            (row_send.at[some_cols], ROWS),
            (gt.at[some_cols], GATE), (p_out.at[some_cols], PART), (sg_out.at[some_cols], SLOT)]
    if n_head > 1:
        sent += [
            (logit.at[others], LOGIT), (x_all.at[others], XALL), (gh_all.at[others], GH),
            (inner_v.at[others], INNER),
        ]
    gg_copy.wait_send()
    across_copy.wait_send()
    s_copy.wait_send()
    for ref, which in sent:
        drain(ref, send_sem.at[which])
    if n_head > 1:
        drain(q_in.at[others], qr)
        drain(kv_in.at[others], kvr)
    span = heads * HEAD_WIDTH
    for i in range(n_head):
        gq_out[:, i * span : (i + 1) * span] = q_in[i]
    replicas = n_head // KEY_VALUE_HEADS
    for g in range(KEY_VALUE_HEADS):
        for k, out in enumerate((gk_out, gv_out)):
            total = kv_in[g * replicas, k].astype(F32)
            for i in range(1, replicas):
                total = total + kv_in[g * replicas + i, k].astype(F32)
            out[:, g * HEAD_WIDTH : (g + 1) * HEAD_WIDTH] = total.astype(BF16)
    if n_head > 1:
        drain(q_send.at[others], send_sem.at[QS])
        drain(kv_send.at[others], send_sem.at[KVS])


def write_out(*refs):
    n = (len(refs) - 1) // 2
    sems = refs[-1]
    copies = [
        pltpu.make_async_copy(refs[i], refs[n + i], sems.at[i]) for i in range(n)
    ]
    for cp in copies:
        cp.start()
    for cp in copies:
        cp.wait()


def solution(mesh):
    n_exp = mesh.shape["exp"]
    n_head = mesh.shape["head"]
    cols = n_exp // 2

    def per_device(
        normed_input, norm_gain, norm_scale, out_grad, router_weight, routed_experts,
        expert_grad, gate_grad, out_proj, query_states, rotated_keys, value_tensor,
    ):
        _, seq, width = normed_input.shape
        experts_all = router_weight.shape[1]
        local, _, cap, _ = expert_grad.shape
        pair = 2 * local
        span, width_total = out_proj.shape
        heads = span // HEAD_WIDTH
        tok = seq // n_head
        kv_width = rotated_keys.shape[2]
        vm = pltpu.VMEM
        dma = pltpu.SemaphoreType.DMA
        vmem = pl.BlockSpec(memory_space=pltpu.VMEM)
        hbm = pl.BlockSpec(memory_space=pltpu.HBM)
        room = -(-cap // 16) * 16
        top_k = routed_experts.shape[2]
        outs = pl.pallas_call(
            functools.partial(kernel, n_exp, n_head, width_total),
            name="moe_attention_backward",
            out_shape=(
                jax.ShapeDtypeStruct((seq, width), BF16),
                jax.ShapeDtypeStruct((tok, n_head * span), BF16),
                jax.ShapeDtypeStruct((tok, kv_width), BF16),
                jax.ShapeDtypeStruct((tok, kv_width), BF16),
            ),
            in_specs=[hbm] * 12,
            out_specs=(vmem,) * 4,
            scratch_shapes=[
                vm((1, width), F32), vm((1, seq), F32),
                vm((seq, width), BF16), vm((experts_all, width), BF16),
                vm((top_k, seq), jnp.int32), vm((local, cap, n_exp, width), BF16),
                vm(gate_grad.shape, BF16), vm((seq, span), BF16),
                vm((seq, kv_width), BF16), vm((seq, kv_width), BF16), dma((11,)),
                vm((n_head, span, width), BF16),
                vm((cols, local * room, width), BF16),
                vm((cols, 2, local * room, width), BF16),
                vm(gate_grad.shape, BF16),
                vm((n_head, experts_all, seq), F32),
                vm((cols, pair, seq), F32),
                vm((cols, pair, seq), F32),
                vm((cols, seq, width), BF16),
                vm((cols, seq, width), BF16),
                vm((cols, pair, seq), F32),
                vm((cols, pair, seq), F32),
                vm((experts_all, seq), F32),
                vm((n_head, seq, HEAD_WIDTH), F32),
                vm((n_head, 2, seq, width // 2), BF16),
                vm((n_head, seq, width), BF16),
                vm((2 * seq, span), F32),
                vm((heads * seq, seq), F32),
                vm((n_head, tok, span), BF16),
                vm((n_head, tok, span), BF16),
                vm((n_head, 2, tok, HEAD_WIDTH), BF16),
                vm((n_head, 2, tok, HEAD_WIDTH), BF16),
                vm((local, seq), F32), vm((local, seq), F32),
                vm((seq, width), BF16), vm((seq, width), BF16),
                dma, dma((13,)), dma((cols,)), dma, dma, dma((cols,)), dma((cols,)), dma,
                dma, dma((n_head, 2)), dma, dma, dma, dma, dma,
                pltpu.SemaphoreType.REGULAR, pltpu.SemaphoreType.REGULAR,
            ],
            compiler_params=pltpu.CompilerParams(
                collective_id=0, has_side_effects=True, vmem_limit_bytes=48 * 1024 * 1024
            ),
        )(
            *(
                pltpu.with_memory_space_constraint(a, pltpu.HBM)
                for a in (
                    normed_input[0], norm_gain[None], norm_scale, out_grad[0], router_weight.T,
                    routed_experts[0].T, jnp.transpose(expert_grad, (0, 2, 1, 3)), gate_grad,
                    out_proj, query_states[0], rotated_keys[0], value_tensor[0],
                )
            )
        )
        outs = pl.pallas_call(
            write_out,
            name="write_out",
            out_shape=tuple(jax.ShapeDtypeStruct(o.shape, o.dtype) for o in outs),
            in_specs=[vmem] * 4,
            out_specs=(hbm,) * 4,
            scratch_shapes=[dma((4,))],
            compiler_params=pltpu.CompilerParams(vmem_limit_bytes=1024 * 1024),
        )(*outs)
        return tuple(o[None] for o in outs)

    placed = (
        P("exp", None, "head"),
        P("head"),
        P("exp", None),
        P("exp", None, "head"),
        P("head", None),
        P("exp", None, None),
        P("exp", None, None, "head"),
        P("exp", None, None),
        P("head", None),
        P("exp", None, "head"),
        P("exp", None, None),
        P("exp", None, None),
    )
    return jax.shard_map(
        per_device,
        mesh=mesh,
        in_specs=placed,
        out_specs=(
            P("exp", None, "head"),
            P("exp", "head", None),
            P("exp", "head", None),
            P("exp", "head", None),
        ),
        check_vma=False,
    )
```

```python
import functools
import math

import jax
import jax.numpy as jnp
from jax import lax
from jax.experimental import pallas as pl
from jax.experimental.pallas import tpu as pltpu
from jax.sharding import PartitionSpec as P

QUERY_HEADS = 64
KEY_VALUE_HEADS = 4
HEAD_WIDTH = 128
MESH = pl.DeviceIdType.MESH
NT = (((1,), (1,)), ((), ()))
TN = (((0,), (0,)), ((), ()))
F32 = jnp.float32
BF16 = jnp.bfloat16


def mm(a, b, dims=(((1,), (0,)), ((), ()))):
    return lax.dot_general(a, b, dims, preferred_element_type=F32)


def kernel(
    n_exp, n_head, width_total,
    x_hbm, gain_hbm, scale_hbm, og_hbm, router_hbm, ids_hbm, expert_hbm, gg_hbm, proj_ref,
    q_hbm, k_hbm, v_hbm,
    gh_out, gq_out, gk_out, gv_out,
    gain_ref, scale_ref, og_ref, router_ref, ids_ref, expert_ref, gg_ref,
    q_ref, k_ref, v_ref, in_sem,
    w_v, row_send, rows, gg_in, logit, gt, gates, p_out, p_in, sg_out, sg_in, diff_v, inner_v, gh_all, x_all,
    ctx, probs_v, q_send, q_in, kv_send, kv_in, across, across_out, s_out, s_in, diag_in, diag_out, far_out, far_in, spread_v, grad_v,
    w_sem, send_sem, xr, ggr, lr, gr, pr, sr, inr, hr, xar, qr, kvr, acr, shr, dgr, fr, up_sem, down_sem, side_sem,
):
    e = lax.axis_index("exp")
    h = lax.axis_index("head")
    x = lax.rem(e, 2)
    z = e // 2
    cols = n_exp // 2
    seq, width = x_all.shape[1:]
    experts_all = router_ref.shape[0]
    local, cap = expert_ref.shape[:2]
    room = rows.shape[2] // local
    pair = 2 * local
    heads = proj_ref.shape[0] // HEAD_WIDTH
    tok = seq // n_head
    half = width // 2
    partner = 2 * z + 1 - x
    ROWS, GG, LOGIT, GATE, PART, SLOT, GH, INNER, XALL, QS, KVS, ACROSS, SHARE, FAR, DIAG = range(15)

    def exp_peer(i):
        return {"exp": 2 * i + x}

    def send(src, dst, s_sem, r_sem, to):
        return pltpu.make_async_remote_copy(
            src_ref=src, dst_ref=dst, send_sem=send_sem.at[s_sem], recv_sem=r_sem,
            device_id=to, device_id_type=MESH,
        )

    def drain(ref, sem):
        pltpu.make_async_copy(ref, ref, sem).wait()

    chips = n_head // 2
    chip, core = h // 2, lax.rem(h, 2)
    sibling = 2 * chip + 1 - core
    same, cross = [], []
    for i in range(1, chips):
        there = 2 * lax.rem(chip + i, chips)
        same.append(there + core)
        cross.append(there + 1 - core)
    head_peers = [sibling] + same + cross
    paired = cols > 1
    if paired:
        edge = z // (cols - 1)
        near = z + 1 - 2 * edge
        row_cols = [i + 2 * ((i + cols - z + edge) // cols) for i in range(cols - 2)]
        col_peers = [near] + row_cols
    else:
        row_cols = []
        col_peers = []
    all_cols = row_cols + ([near] if paired else []) + [z]

    barrier = pltpu.get_barrier_semaphore()
    pl.semaphore_signal(barrier, inc=1, device_id={"exp": partner}, device_id_type=MESH)
    for p in head_peers:
        pl.semaphore_signal(barrier, inc=1, device_id={"head": p}, device_id_type=MESH)

    @pl.when(z > 0)
    def _():
        pl.semaphore_signal(barrier, inc=1, device_id=exp_peer(z - 1), device_id_type=MESH)

    @pl.when(z < cols - 1)
    def _():
        pl.semaphore_signal(barrier, inc=1, device_id=exp_peer(z + 1), device_id_type=MESH)

    greeted = 1 + (n_head - 1) + (z + cols - 1) // cols + (2 * cols - 2 - z) // cols

    loads = {}
    for i, (name, src, dst) in enumerate((
        ("expert", expert_hbm, expert_ref), ("x", x_hbm, x_all.at[h]), ("gain", gain_hbm, gain_ref),
        ("router", router_hbm, router_ref), ("gg", gg_hbm, gg_ref), ("ids", ids_hbm, ids_ref),
        ("q", q_hbm, q_ref), ("k", k_hbm, k_ref), ("v", v_hbm, v_ref), ("og", og_hbm, og_ref),
        ("scale", scale_hbm, scale_ref),
    )):
        loads[name] = pltpu.make_async_copy(src, dst, in_sem.at[i])
    for cp in loads.values():
        cp.start()
    w_copies = [
        pltpu.make_async_copy(proj_ref.at[:, pl.ds(j * width, width)], w_v.at[j], w_sem)
        for j in range(n_head)
    ]

    loads["expert"].wait()
    flat = expert_ref.reshape(local, cap * n_exp, width)

    def pick(c_list, side):
        m = len(c_list) * room
        r_i = lax.broadcasted_iota(jnp.int32, (m, cap * n_exp), 0)
        k_i = lax.broadcasted_iota(jnp.int32, (m, cap * n_exp), 1)
        group = r_i // room
        number = jnp.zeros_like(r_i)
        for i, c in enumerate(c_list):
            number = jnp.where(group == i, 2 * c + side, number)
        slot = r_i - group * room
        one = jnp.logical_and(slot < cap, slot * n_exp + number == k_i)
        return jnp.where(one, 1.0, 0.0).astype(BF16)

    def row_copy(c, j):
        part = pl.ds(j * room, room)
        return send(row_send.at[c, part], rows.at[c, 1, part], ROWS, xr.at[c], {"exp": partner})

    row_order = [(c, j) for c in row_cols for j in range(local)]
    held = len(row_order) - len(row_order) // 4
    step = min(cols, 4)

    def pick_all(side, into):
        for first in range(0, cols, step):
            some = all_cols[first : first + step]
            chosen = pick(some, side)
            for j in range(local):
                got = mm(chosen, flat[j]).astype(BF16)
                for i, c in enumerate(some):
                    into(c)[j * room : (j + 1) * room] = got[i * room : (i + 1) * room]

    pick_all(1 - x, lambda c: row_send.at[c])
    loads["gg"].wait()
    pl.semaphore_wait(barrier, greeted)
    gg_copy = send(gg_ref, gg_in, GG, ggr, {"exp": partner})
    gg_copy.start()
    for c, j in row_order[:held]:
        row_copy(c, j).start()
    if paired:
        pl.semaphore_signal(side_sem, inc=1, device_id={"exp": partner}, device_id_type=MESH)
    if cols > 2:
        @pl.when(z == 1)
        def _():
            pl.semaphore_signal(up_sem, inc=1, device_id=exp_peer(z + 1), device_id_type=MESH)

        @pl.when(z == cols - 2)
        def _():
            pl.semaphore_signal(down_sem, inc=1, device_id=exp_peer(z - 1), device_id_type=MESH)

    for name in ("x", "gain", "router"):
        loads[name].wait()
    gain = gain_ref[...]

    def hidden_f32():
        return x_all[h].astype(F32)

    logit[h] = mm(router_ref[...], (hidden_f32() * gain).astype(BF16), NT)

    def logit_copy(src, to):
        return send(logit.at[src], logit.at[src], LOGIT, lr, {"head": to})

    def x_copy(src, to):
        return send(x_all.at[src], x_all.at[src], XALL, xar, {"head": to})

    for p in head_peers:
        logit_copy(h, p).start()
    for p in head_peers:
        x_copy(h, p).start()
    for cp in w_copies:
        cp.start()

    pick_all(x, lambda c: rows.at[c, 0])

    if paired:
        pl.semaphore_wait(side_sem, 1)
    if cols > 3:
        @pl.when(jnp.logical_and(z > 1, z < cols - 1))
        def _():
            pl.semaphore_wait(up_sem, 1)
            pl.semaphore_signal(up_sem, inc=1, device_id=exp_peer(z + 1), device_id_type=MESH)

        @pl.when(jnp.logical_and(z > 0, z < cols - 2))
        def _():
            pl.semaphore_wait(down_sem, 1)
            pl.semaphore_signal(down_sem, inc=1, device_id=exp_peer(z - 1), device_id_type=MESH)

    for name in ("ids", "q", "k", "v"):
        loads[name].wait()
    kv = h * heads // (QUERY_HEADS // KEY_VALUE_HEADS)
    lanes = pl.ds(pl.multiple_of(kv * HEAD_WIDTH, HEAD_WIDTH), HEAD_WIDTH)

    def stacked(a):
        return jnp.concatenate(
            [a[:, i * HEAD_WIDTH : (i + 1) * HEAD_WIDTH] for i in range(a.shape[1] // HEAD_WIDTH)],
            axis=0,
        )

    inv_sqrt = 1.0 / math.sqrt(HEAD_WIDTH)
    scores = mm(stacked(q_ref[...]), k_ref[:, lanes], NT) * inv_sqrt
    position = lax.rem(lax.broadcasted_iota(jnp.int32, scores.shape, 0), seq)
    causal = position >= lax.broadcasted_iota(jnp.int32, scores.shape, 1)
    scores = jnp.where(causal, scores, -jnp.inf)
    probs = jnp.exp(scores - jnp.max(scores, axis=1, keepdims=True))
    probs_v[...] = probs / jnp.sum(probs, axis=1, keepdims=True)

    expert_i = lax.broadcasted_iota(jnp.int32, (experts_all, seq), 0)
    member = ids_ref[0:1] == expert_i
    for i in range(1, ids_ref.shape[0]):
        member = jnp.logical_or(member, ids_ref[i : i + 1] == expert_i)
    row_i = lax.broadcasted_iota(jnp.int32, (seq, seq), 0)
    col_i = lax.broadcasted_iota(jnp.int32, (seq, seq), 1)

    if n_head > 1:
        drain(logit.at[pl.ds(0, n_head - 1)], lr)
    total = logit[0]
    for i in range(1, n_head):
        total = total + logit[i]
    total = jnp.where(member, total, -jnp.inf)
    top = jnp.max(total, axis=0, keepdims=True)
    weights = jnp.exp(total - top)
    weights = weights / jnp.sum(weights, axis=0, keepdims=True)
    weights_t = jnp.where(member, weights, -1.0)
    for c in range(cols):
        gt[c] = weights_t[c * pair : (c + 1) * pair]

    def gate_copy(c):
        return send(gt.at[c], gates.at[z], GATE, gr.at[z], exp_peer(c))

    def gate_wait(c):
        return send(gt.at[c], gates.at[c], GATE, gr.at[c], exp_peer(c))

    def by_side(a):
        low, high = a[:local], a[local:]
        return jnp.where(x == 0, low, high), jnp.where(x == 0, high, low)

    def far():
        if cols > 2:
            @pl.when(z == 0)
            def _():
                pl.semaphore_wait(down_sem, 1)

            @pl.when(z == cols - 1)
            def _():
                pl.semaphore_wait(up_sem, 1)

    askers = [(z > 0, z - 1), (z == cols - 2, z + 1)]

    def across_of(c):
        return {"exp": 2 * c + 1 - x}

    def diag_copy(k, to):
        return send(diag_out.at[k], diag_in, DIAG + k, dgr, across_of(to))

    def far_copy(k, to):
        return send(far_out, far_in.at[k], FAR, fr.at[k], across_of(to))

    across_out[...] = by_side(gt[z])[1]
    across_copy = send(across_out, across, ACROSS, acr, {"exp": partner})
    across_copy.start()
    if paired:
        for k, (on, to) in enumerate(askers):
            @pl.when(on)
            def _():
                diag_out[k] = by_side(gt[to])[1]
                diag_copy(k, to).start()
        gate_copy(near).start()
    for c, j in row_order[held:]:
        row_copy(c, j).start()
    far()
    for c in row_cols:
        gate_copy(c).start()

    earlier = (row_i < col_i).astype(BF16)
    slot_i = lax.broadcasted_iota(jnp.int32, (room, seq), 0)
    seq_i = lax.broadcasted_iota(jnp.int32, (n_exp, seq), 0)
    gg_copy.wait_recv()

    def places(w):
        named = w >= 0.0
        before = mm(jnp.where(named, 1.0, 0.0).astype(BF16), earlier).astype(jnp.int32)
        hits = []
        for j in range(w.shape[0]):
            hits.append(jnp.logical_and(before[j : j + 1] == slot_i, named[j : j + 1]))
        spread = [jnp.where(hit, w[j : j + 1], 0.0).astype(BF16) for j, hit in enumerate(hits)]
        return spread, hits

    def contribution(c, w, into):
        spread, hits = places(jnp.concatenate(by_side(w), axis=0))
        slots = []
        for j in range(pair):
            table = (gg_ref if j < local else gg_in)[j % local]
            by_seq = mm(table, jnp.where(hits[j][:cap], 1.0, 0.0).astype(BF16))
            slots.append(
                jnp.sum(jnp.where(seq_i == 2 * c + x, by_seq, 0.0), axis=0, keepdims=True)
            )
        for j in range(pair):
            into[c, j : j + 1] = jnp.where(x == 0, slots[j], slots[(j + local) % pair])
        return jnp.concatenate(spread, axis=0)

    def row_wait(c):
        drain(rows.at[c, 1], xr.at[c])

    s_copy = send(s_out, s_in, SHARE, shr, {"exp": partner})

    def share():
        if paired:
            diag_copy(0, near).wait_recv()
            far_out[...] = shared(diag_in[...], near)
            far_copy(edge, near).start()
        across_copy.wait_recv()
        s_out[...] = shared(across[...], z)
        s_copy.start()

    def part_copy(c):
        return send(p_out.at[c], p_in.at[z], PART, pr.at[z], exp_peer(c))

    def slot_copy(c):
        return send(sg_out.at[c], sg_in.at[z], SLOT, sr, exp_peer(c))

    spread_z = contribution(z, gt[z], sg_in)
    grad = mm(spread_z[: local * room], rows[z, 0], TN)
    def slots_to(c, k):
        gate_wait(c).wait_recv()
        spread_v[k] = contribution(c, gates[c], sg_out)
        slot_copy(c).start()

    def shared(w, c):
        return mm(jnp.concatenate(places(w)[0], axis=0), row_send[c], TN).astype(BF16)

    def whole_part(c, k):
        row_wait(c)
        p_out[c] = mm(spread_v[k], rows[c].reshape(pair * room, width), TN).astype(BF16)
        part_copy(c).start()

    last = len(row_cols)

    def near_part():
        slots_to(near, last)
        p_out[near] = mm(spread_v[last][: local * room], rows[near, 0], TN).astype(BF16)
        part_copy(near).start()

    def later_slots():
        for k in range(1, last):
            slots_to(row_cols[k], k)

    low = z < cols // 2
    high = z >= cols // 2
    if paired:
        pl.when(z == 0)(near_part)
    if row_cols:
        slots_to(row_cols[0], 0)
        whole_part(row_cols[0], 0)
    if paired:
        pl.when(high)(later_slots)
        pl.when(z > 0)(near_part)
    share()
    if paired:
        pl.when(low)(later_slots)
    else:
        later_slots()
    for k in range(1, last):
        whole_part(row_cols[k], k)
    if cols > 1:
        drain(sg_in.at[pl.ds(0, cols - 1)], sr)
    mean = jnp.zeros((1, seq), F32)
    for c in range(cols):
        mean = mean + jnp.sum(jnp.maximum(gt[c], 0.0) * sg_in[c], axis=0, keepdims=True)
    for c in range(cols):
        diff_v[c * pair : (c + 1) * pair] = jnp.maximum(gt[c], 0.0) * (sg_in[c] - mean)
    diff = diff_v[...]
    diff_hi = diff.astype(BF16)
    diff_lo = (diff - diff_hi.astype(F32)).astype(BF16)
    grad = grad + mm(diff_hi, router_ref[...], TN) + mm(diff_lo, router_ref[...], TN)
    loads["og"].wait()
    loads["scale"].wait()
    scale = jnp.sum(
        jnp.where(row_i == col_i, jnp.broadcast_to(scale_ref[...], (seq, seq)), 0.0),
        axis=1, keepdims=True,
    )
    s_copy.wait_recv()
    grad = grad + s_in[...].astype(F32)
    if paired:
        grad_v[...] = grad
        for k, (on, to) in enumerate(askers):
            @pl.when(on)
            def _():
                far_copy(k, to).wait_recv()
                grad_v[...] = grad_v[...] + far_in[k].astype(F32)
        grad = grad_v[...]
    for i, c in enumerate(col_peers):
        drain(p_in.at[c], pr.at[c])
        grad = grad + p_in[c].astype(F32)


    def gh_copy(src, k, to):
        return send(
            gh_all.at[src, k], gh_all.at[src, k], GH, hr.at[src, k], {"head": to}
        )

    def half_of(a, k):
        return a[:, k * half : (k + 1) * half]

    base = []
    for k in range(2):
        base.append(
            half_of(og_ref[...], k).astype(F32) + scale * (half_of(gain, k) * half_of(grad, k))
        )
        gh_all[h, k] = base[k].astype(BF16)
        for p in [sibling] + same:
            gh_copy(h, k, p).start()
    for p in cross:
        for k in range(2):
            gh_copy(h, k, p).start()
    inner_v[h] = jnp.broadcast_to(
        jnp.sum(hidden_f32() * gain * grad, axis=1, keepdims=True), (seq, HEAD_WIDTH)
    )

    def inner_copy(src, to):
        return send(inner_v.at[src], inner_v.at[src], INNER, inr, {"head": to})

    for p in head_peers:
        inner_copy(h, p).start()
    drain(w_v, w_sem)
    if n_head > 1:
        drain(x_all.at[pl.ds(0, n_head - 1)], xar)

    rows_w = w_v.shape[1]
    tile = min(512, rows_w)
    group = max(rows_w // 2, HEAD_WIDTH)
    per = group // HEAD_WIDTH

    def piece(p, k):
        return (
            jnp.concatenate([gh_all[p, k], x_all[p, :, k * half : (k + 1) * half]], axis=0),
            k * half, half,
        )

    def whole(p):
        return (
            jnp.concatenate(
                [jnp.concatenate([gh_all[p, 0], gh_all[p, 1]], axis=1), x_all[p]], axis=0
            ),
            0, width,
        )

    def product(p, block, r):
        a, at, size = block
        return mm(a, w_v[p, r : r + tile, at : at + size], NT)

    stages = [(h, None)] + [(sibling, None)]
    for p in same + cross:
        stages += [(p, 0), (p, 1)]
    for i, (p, k) in enumerate(stages[:-1]):
        if i:
            for kk in (0, 1) if k is None else (k,):
                drain(gh_all.at[p, kk], hr.at[p, kk])
        block = whole(p) if k is None else piece(p, k)
        for r in range(0, rows_w, tile):
            part = product(p, block, r)
            if i:
                part = ctx[:, r : r + tile] + part
            ctx[:, r : r + tile] = part

    if n_head > 1:
        drain(inner_v.at[pl.ds(0, n_head - 1)], inr)
    inner = inner_v[0]
    for i in range(1, n_head):
        inner = inner + inner_v[i]
    taken = scale * inner[:, 0:1] / width_total

    p, k = stages[-1]
    if k is None:
        for kk in (0, 1):
            drain(gh_all.at[p, kk], hr.at[p, kk])
        block = whole(p)
    else:
        drain(gh_all.at[p, k], hr.at[p, k])
        block = piece(p, k)
    key_block = k_ref[:, lanes]
    value_block = v_ref[:, lanes]
    gk = jnp.zeros((seq, HEAD_WIDTH), F32)
    gv = jnp.zeros((seq, HEAD_WIDTH), F32)

    def q_copy(r, to):
        at = pl.ds(r, group)
        return send(q_send.at[to, :, at], q_in.at[h, :, at], QS, qr, {"head": to})

    def kv_copy(to):
        return send(kv_send.at[to], kv_in.at[h], KVS, kvr, {"head": to})

    def finish(r):
        for t in range(r, r + group, min(tile, group)):
            size = min(tile, group)
            a, at, depth = block
            ctx[:, t : t + size] = ctx[:, t : t + size] + mm(
                a, w_v[p, t : t + size, at : at + depth], NT
            )

    def back(r):
        part = ctx[:, r : r + group]
        ctx_s = stacked((part[:seq] - taken * part[seq:]).astype(BF16))
        first = r // HEAD_WIDTH
        probs = probs_v[first * seq : (first + per) * seq]
        prob_grads = mm(ctx_s, value_block, NT)
        delta = jnp.sum(probs * prob_grads, axis=1, keepdims=True)
        score_grads = (probs * (prob_grads - delta) * inv_sqrt).astype(BF16)
        gq = mm(score_grads, key_block).astype(BF16)
        for d in range(n_head):
            for i in range(per):
                s = i * seq + d * tok
                q_send[d, :, r + i * HEAD_WIDTH : r + (i + 1) * HEAD_WIDTH] = gq[s : s + tok]
        return score_grads, probs.astype(BF16), ctx_s

    def depart(r):
        for to in head_peers:
            q_copy(r, to).start()

    groups = list(range(0, rows_w, group))
    kept = []
    finish(groups[0])
    for i, r in enumerate(groups):
        kept.append(back(r))
        if i + 1 < len(groups):
            finish(groups[i + 1])
        depart(r)
    for r, (score_grads, probs, ctx_s) in zip(groups, kept):
        gk = gk + mm(score_grads, stacked(q_ref[:, r : r + group]), TN)
        gv = gv + mm(probs, ctx_s, TN)
    for d in range(n_head):
        kv_send[d, 0] = gk[d * tok : (d + 1) * tok].astype(BF16)
        kv_send[d, 1] = gv[d * tok : (d + 1) * tok].astype(BF16)
    for to in head_peers:
        kv_copy(to).start()
    for k in range(2):
        gh_out[:, k * half : (k + 1) * half] = (
            base[k] - half_of(hidden_f32(), k) * taken
        ).astype(BF16)
    q_in[h] = q_send[h]
    kv_in[h] = kv_send[h]

    others = pl.ds(0, n_head - 1)
    some_cols = pl.ds(0, cols - 1)
    sent = []
    if row_cols:
        sent += [(row_send.at[pl.ds(0, len(row_cols))], ROWS)]
    if paired:
        far_copy(edge, near).wait_send()
        for k, (on, to) in enumerate(askers):
            @pl.when(on)
            def _():
                diag_copy(k, to).wait_send()
    if cols > 1:
        sent += [(gt.at[some_cols], GATE), (p_out.at[some_cols], PART), (sg_out.at[some_cols], SLOT)]
    if n_head > 1:
        sent += [
            (logit.at[others], LOGIT), (x_all.at[others], XALL), (gh_all.at[others], GH),
            (inner_v.at[others], INNER),
        ]
    gg_copy.wait_send()
    across_copy.wait_send()
    s_copy.wait_send()
    for ref, which in sent:
        drain(ref, send_sem.at[which])
    if n_head > 1:
        drain(q_in.at[others], qr)
        drain(kv_in.at[others], kvr)
    span = heads * HEAD_WIDTH
    for i in range(n_head):
        gq_out[:, i * span : (i + 1) * span] = q_in[i]
    replicas = n_head // KEY_VALUE_HEADS
    for g in range(KEY_VALUE_HEADS):
        for k, out in enumerate((gk_out, gv_out)):
            total = kv_in[g * replicas, k].astype(F32)
            for i in range(1, replicas):
                total = total + kv_in[g * replicas + i, k].astype(F32)
            out[:, g * HEAD_WIDTH : (g + 1) * HEAD_WIDTH] = total.astype(BF16)
    if n_head > 1:
        drain(q_send.at[others], send_sem.at[QS])
        drain(kv_send.at[others], send_sem.at[KVS])


def write_out(*refs):
    n = (len(refs) - 1) // 2
    sems = refs[-1]
    copies = [
        pltpu.make_async_copy(refs[i], refs[n + i], sems.at[i]) for i in range(n)
    ]
    for cp in copies:
        cp.start()
    for cp in copies:
        cp.wait()


def solution(mesh):
    n_exp = mesh.shape["exp"]
    n_head = mesh.shape["head"]
    cols = n_exp // 2

    def per_device(
        normed_input, norm_gain, norm_scale, out_grad, router_weight, routed_experts,
        expert_grad, gate_grad, out_proj, query_states, rotated_keys, value_tensor,
    ):
        _, seq, width = normed_input.shape
        experts_all = router_weight.shape[1]
        local, _, cap, _ = expert_grad.shape
        pair = 2 * local
        span, width_total = out_proj.shape
        heads = span // HEAD_WIDTH
        tok = seq // n_head
        kv_width = rotated_keys.shape[2]
        vm = pltpu.VMEM
        dma = pltpu.SemaphoreType.DMA
        vmem = pl.BlockSpec(memory_space=pltpu.VMEM)
        hbm = pl.BlockSpec(memory_space=pltpu.HBM)
        room = -(-cap // 16) * 16
        top_k = routed_experts.shape[2]
        outs = pl.pallas_call(
            functools.partial(kernel, n_exp, n_head, width_total),
            name="moe_attention_backward",
            out_shape=(
                jax.ShapeDtypeStruct((seq, width), BF16),
                jax.ShapeDtypeStruct((tok, n_head * span), BF16),
                jax.ShapeDtypeStruct((tok, kv_width), BF16),
                jax.ShapeDtypeStruct((tok, kv_width), BF16),
            ),
            in_specs=[hbm] * 12,
            out_specs=(vmem,) * 4,
            scratch_shapes=[
                vm((1, width), F32), vm((1, seq), F32),
                vm((seq, width), BF16), vm((experts_all, width), BF16),
                vm((top_k, seq), jnp.int32), vm((local, cap, n_exp, width), BF16),
                vm(gate_grad.shape, BF16), vm((seq, span), BF16),
                vm((seq, kv_width), BF16), vm((seq, kv_width), BF16), dma((11,)),
                vm((n_head, span, width), BF16),
                vm((cols, local * room, width), BF16),
                vm((cols, 2, local * room, width), BF16),
                vm(gate_grad.shape, BF16),
                vm((n_head, experts_all, seq), F32),
                vm((cols, pair, seq), F32),
                vm((cols, pair, seq), F32),
                vm((cols, seq, width), BF16),
                vm((cols, seq, width), BF16),
                vm((cols, pair, seq), F32),
                vm((cols, pair, seq), F32),
                vm((experts_all, seq), F32),
                vm((n_head, seq, HEAD_WIDTH), F32),
                vm((n_head, 2, seq, width // 2), BF16),
                vm((n_head, seq, width), BF16),
                vm((2 * seq, span), F32),
                vm((heads * seq, seq), F32),
                vm((n_head, tok, span), BF16),
                vm((n_head, tok, span), BF16),
                vm((n_head, 2, tok, HEAD_WIDTH), BF16),
                vm((n_head, 2, tok, HEAD_WIDTH), BF16),
                vm((local, seq), F32), vm((local, seq), F32),
                vm((seq, width), BF16), vm((seq, width), BF16),
                vm((local, seq), F32), vm((2, local, seq), F32),
                vm((seq, width), BF16), vm((2, seq, width), BF16),
                vm((max(cols - 1, 1), pair * room, seq), BF16), vm((seq, width), F32),
                dma, dma((16,)), dma((cols,)), dma, dma, dma((cols,)), dma((cols,)), dma,
                dma, dma((n_head, 2)), dma, dma, dma, dma, dma, dma, dma((2,)),
                pltpu.SemaphoreType.REGULAR, pltpu.SemaphoreType.REGULAR,
                pltpu.SemaphoreType.REGULAR,
            ],
            compiler_params=pltpu.CompilerParams(
                collective_id=0, has_side_effects=True, vmem_limit_bytes=48 * 1024 * 1024
            ),
        )(
            *(
                pltpu.with_memory_space_constraint(a, pltpu.HBM)
                for a in (
                    normed_input[0], norm_gain[None], norm_scale, out_grad[0], router_weight.T,
                    routed_experts[0].T, jnp.transpose(expert_grad, (0, 2, 1, 3)), gate_grad,
                    out_proj, query_states[0], rotated_keys[0], value_tensor[0],
                )
            )
        )
        outs = pl.pallas_call(
            write_out,
            name="write_out",
            out_shape=tuple(jax.ShapeDtypeStruct(o.shape, o.dtype) for o in outs),
            in_specs=[vmem] * 4,
            out_specs=(hbm,) * 4,
            scratch_shapes=[dma((4,))],
            compiler_params=pltpu.CompilerParams(vmem_limit_bytes=1024 * 1024),
        )(*outs)
        return tuple(o[None] for o in outs)

    placed = (
        P("exp", None, "head"),
        P("head"),
        P("exp", None),
        P("exp", None, "head"),
        P("head", None),
        P("exp", None, None),
        P("exp", None, None, "head"),
        P("exp", None, None),
        P("head", None),
        P("exp", None, "head"),
        P("exp", None, None),
        P("exp", None, None),
    )
    return jax.shard_map(
        per_device,
        mesh=mesh,
        in_specs=placed,
        out_specs=(
            P("exp", None, "head"),
            P("exp", "head", None),
            P("exp", "head", None),
            P("exp", "head", None),
        ),
        check_vma=False,
    )
```

```python
import functools
import math

import jax
import jax.numpy as jnp
from jax import lax
from jax.experimental import pallas as pl
from jax.experimental.pallas import tpu as pltpu
from jax.sharding import PartitionSpec as P

QUERY_HEADS = 64
KEY_VALUE_HEADS = 4
HEAD_WIDTH = 128
MESH = pl.DeviceIdType.MESH
NT = (((1,), (1,)), ((), ()))
TN = (((0,), (0,)), ((), ()))
F32 = jnp.float32
BF16 = jnp.bfloat16


def mm(a, b, dims=(((1,), (0,)), ((), ()))):
    return lax.dot_general(a, b, dims, preferred_element_type=F32)


def kernel(
    n_exp, n_head, width_total,
    x_hbm, gain_hbm, scale_hbm, og_hbm, router_hbm, ids_hbm, expert_hbm, gg_hbm, proj_ref,
    q_hbm, k_hbm, v_hbm,
    gh_out, gq_out, gk_out, gv_out,
    gain_ref, scale_ref, og_ref, router_ref, ids_ref, expert_ref, gg_all,
    q_ref, k_ref, v_ref, in_sem,
    w_v, row_send, rows, logit, gt, gates, p_out, p_in, inner_v, gh_all, x_all,
    ctx, probs_v, q_send, q_in, kv_send, kv_in, across, across_out, s_out, s_in, diag_in, diag_out, far_out, far_in, near_in, spread_v, grad_v,
    w_sem, send_sem, xr, ggr, lr, gr, pr, ggzr, inr, hr, xar, qr, kvr, acr, shr, dgr, fr, nr, up_sem, down_sem, side_sem,
):
    e = lax.axis_index("exp")
    h = lax.axis_index("head")
    x = lax.rem(e, 2)
    z = e // 2
    cols = n_exp // 2
    seq, width = x_all.shape[1:]
    experts_all = router_ref.shape[0]
    local, cap = expert_ref.shape[:2]
    room = rows.shape[2] // local
    pair = 2 * local
    heads = proj_ref.shape[0] // HEAD_WIDTH
    tok = seq // n_head
    half = width // 2
    partner = 2 * z + 1 - x
    ROWS, GG, LOGIT, GATE, PART, GGZ, GH, INNER, XALL, QS, KVS, ACROSS, SHARE, FAR, NEAR, DIAG = range(16)

    def exp_peer(i):
        return {"exp": 2 * i + x}

    def send(src, dst, s_sem, r_sem, to):
        return pltpu.make_async_remote_copy(
            src_ref=src, dst_ref=dst, send_sem=send_sem.at[s_sem], recv_sem=r_sem,
            device_id=to, device_id_type=MESH,
        )

    def drain(ref, sem):
        pltpu.make_async_copy(ref, ref, sem).wait()

    chips = n_head // 2
    chip, core = h // 2, lax.rem(h, 2)
    sibling = 2 * chip + 1 - core
    same, cross = [], []
    for i in range(1, chips):
        there = 2 * lax.rem(chip + i, chips)
        same.append(there + core)
        cross.append(there + 1 - core)
    head_peers = [sibling] + same + cross
    paired = cols > 1
    if paired:
        edge = z // (cols - 1)
        near = z + 1 - 2 * edge
        row_cols = [i + 2 * ((i + cols - z + edge) // cols) for i in range(cols - 2)]
        col_peers = [near] + row_cols
    else:
        row_cols = []
        col_peers = []
    all_cols = row_cols + ([near] if paired else []) + [z]

    barrier = pltpu.get_barrier_semaphore()
    pl.semaphore_signal(barrier, inc=1, device_id={"exp": partner}, device_id_type=MESH)
    for p in head_peers:
        pl.semaphore_signal(barrier, inc=1, device_id={"head": p}, device_id_type=MESH)

    @pl.when(z > 0)
    def _():
        pl.semaphore_signal(barrier, inc=1, device_id=exp_peer(z - 1), device_id_type=MESH)

    @pl.when(z < cols - 1)
    def _():
        pl.semaphore_signal(barrier, inc=1, device_id=exp_peer(z + 1), device_id_type=MESH)

    greeted = 1 + (n_head - 1) + (z + cols - 1) // cols + (2 * cols - 2 - z) // cols

    loads = {}
    for i, (name, src, dst) in enumerate((
        ("expert", expert_hbm, expert_ref), ("x", x_hbm, x_all.at[h]), ("gain", gain_hbm, gain_ref),
        ("router", router_hbm, router_ref), ("gg", gg_hbm, gg_all.at[z, x]), ("ids", ids_hbm, ids_ref),
        ("q", q_hbm, q_ref), ("k", k_hbm, k_ref), ("v", v_hbm, v_ref), ("og", og_hbm, og_ref),
        ("scale", scale_hbm, scale_ref),
    )):
        loads[name] = pltpu.make_async_copy(src, dst, in_sem.at[i])
    for cp in loads.values():
        cp.start()
    w_copies = [
        pltpu.make_async_copy(proj_ref.at[:, pl.ds(j * width, width)], w_v.at[j], w_sem)
        for j in range(n_head)
    ]

    loads["expert"].wait()
    flat = expert_ref.reshape(local, cap * n_exp, width)

    def pick(c_list, side):
        m = len(c_list) * room
        r_i = lax.broadcasted_iota(jnp.int32, (m, cap * n_exp), 0)
        k_i = lax.broadcasted_iota(jnp.int32, (m, cap * n_exp), 1)
        group = r_i // room
        number = jnp.zeros_like(r_i)
        for i, c in enumerate(c_list):
            number = jnp.where(group == i, 2 * c + side, number)
        slot = r_i - group * room
        one = jnp.logical_and(slot < cap, slot * n_exp + number == k_i)
        return jnp.where(one, 1.0, 0.0).astype(BF16)

    def row_copy(c, j):
        part = pl.ds(j * room, room)
        return send(row_send.at[c, part], rows.at[c, 1, part], ROWS, xr.at[c], {"exp": partner})

    row_order = [(c, j) for c in row_cols for j in range(local)]
    held = len(row_order) - len(row_order) // 4
    step = min(cols, 4)

    def pick_all(side, into):
        for first in range(0, cols, step):
            some = all_cols[first : first + step]
            chosen = pick(some, side)
            for j in range(local):
                got = mm(chosen, flat[j]).astype(BF16)
                for i, c in enumerate(some):
                    into(c)[j * room : (j + 1) * room] = got[i * room : (i + 1) * room]

    pick_all(1 - x, lambda c: row_send.at[c])
    loads["gg"].wait()
    pl.semaphore_wait(barrier, greeted)
    gg_copy = send(gg_all.at[z, x], gg_all.at[z, x], GG, ggr, {"exp": partner})
    gg_copy.start()
    for c, j in row_order[:held]:
        row_copy(c, j).start()
    if paired:
        pl.semaphore_signal(side_sem, inc=1, device_id={"exp": partner}, device_id_type=MESH)
    if cols > 2:
        @pl.when(z == 1)
        def _():
            pl.semaphore_signal(up_sem, inc=1, device_id=exp_peer(z + 1), device_id_type=MESH)

        @pl.when(z == cols - 2)
        def _():
            pl.semaphore_signal(down_sem, inc=1, device_id=exp_peer(z - 1), device_id_type=MESH)

    for name in ("x", "gain", "router"):
        loads[name].wait()
    gain = gain_ref[...]

    def hidden_f32():
        return x_all[h].astype(F32)

    logit[h] = mm(router_ref[...], (hidden_f32() * gain).astype(BF16), NT)

    def logit_copy(src, to):
        return send(logit.at[src], logit.at[src], LOGIT, lr, {"head": to})

    def x_copy(src, to):
        return send(x_all.at[src], x_all.at[src], XALL, xar, {"head": to})

    for p in head_peers:
        logit_copy(h, p).start()
    for p in head_peers:
        x_copy(h, p).start()
    for cp in w_copies:
        cp.start()

    pick_all(x, lambda c: rows.at[c, 0])

    def near_copy(k, to):
        return send(rows.at[to, 0], near_in.at[k], NEAR, nr.at[k], exp_peer(to))

    if paired:
        near_copy(edge, near).start()

    if paired:
        pl.semaphore_wait(side_sem, 1)
    if cols > 3:
        @pl.when(jnp.logical_and(z > 1, z < cols - 1))
        def _():
            pl.semaphore_wait(up_sem, 1)
            pl.semaphore_signal(up_sem, inc=1, device_id=exp_peer(z + 1), device_id_type=MESH)

        @pl.when(jnp.logical_and(z > 0, z < cols - 2))
        def _():
            pl.semaphore_wait(down_sem, 1)
            pl.semaphore_signal(down_sem, inc=1, device_id=exp_peer(z - 1), device_id_type=MESH)

    for name in ("ids", "q", "k", "v"):
        loads[name].wait()
    kv = h * heads // (QUERY_HEADS // KEY_VALUE_HEADS)
    lanes = pl.ds(pl.multiple_of(kv * HEAD_WIDTH, HEAD_WIDTH), HEAD_WIDTH)

    def stacked(a):
        return jnp.concatenate(
            [a[:, i * HEAD_WIDTH : (i + 1) * HEAD_WIDTH] for i in range(a.shape[1] // HEAD_WIDTH)],
            axis=0,
        )

    inv_sqrt = 1.0 / math.sqrt(HEAD_WIDTH)
    scores = mm(stacked(q_ref[...]), k_ref[:, lanes], NT) * inv_sqrt
    position = lax.rem(lax.broadcasted_iota(jnp.int32, scores.shape, 0), seq)
    causal = position >= lax.broadcasted_iota(jnp.int32, scores.shape, 1)
    scores = jnp.where(causal, scores, -jnp.inf)
    probs = jnp.exp(scores - jnp.max(scores, axis=1, keepdims=True))
    probs_v[...] = probs / jnp.sum(probs, axis=1, keepdims=True)
    ctx[...] = jnp.zeros_like(ctx)

    expert_i = lax.broadcasted_iota(jnp.int32, (experts_all, seq), 0)
    member = ids_ref[0:1] == expert_i
    for i in range(1, ids_ref.shape[0]):
        member = jnp.logical_or(member, ids_ref[i : i + 1] == expert_i)
    row_i = lax.broadcasted_iota(jnp.int32, (seq, seq), 0)
    col_i = lax.broadcasted_iota(jnp.int32, (seq, seq), 1)

    if n_head > 1:
        drain(logit.at[pl.ds(0, n_head - 1)], lr)
    total = logit[0]
    for i in range(1, n_head):
        total = total + logit[i]
    total = jnp.where(member, total, -jnp.inf)
    top = jnp.max(total, axis=0, keepdims=True)
    weights = jnp.exp(total - top)
    weights = weights / jnp.sum(weights, axis=0, keepdims=True)
    weights_t = jnp.where(member, weights, -1.0)
    for c in range(cols):
        gt[c] = weights_t[c * pair : (c + 1) * pair]

    def gate_copy(c):
        return send(gt.at[c], gates.at[z], GATE, gr.at[z], exp_peer(c))

    def gate_wait(c):
        return send(gt.at[c], gates.at[c], GATE, gr.at[c], exp_peer(c))

    def by_side(a):
        low, high = a[:local], a[local:]
        return jnp.where(x == 0, low, high), jnp.where(x == 0, high, low)

    def far():
        if cols > 2:
            @pl.when(z == 0)
            def _():
                pl.semaphore_wait(down_sem, 1)

            @pl.when(z == cols - 1)
            def _():
                pl.semaphore_wait(up_sem, 1)

    askers = [(z > 0, z - 1), (z == cols - 2, z + 1)]

    def across_of(c):
        return {"exp": 2 * c + 1 - x}

    def diag_copy(k, to):
        return send(diag_out.at[k], diag_in, DIAG + k, dgr, across_of(to))

    def far_copy(k, to):
        return send(far_out, far_in.at[k], FAR, fr.at[k], across_of(to))

    across_out[...] = by_side(gt[z])[1]
    across_copy = send(across_out, across, ACROSS, acr, {"exp": partner})
    across_copy.start()
    if paired:
        for k, (on, to) in enumerate(askers):
            @pl.when(on)
            def _():
                diag_out[k] = by_side(gt[to])[1]
                diag_copy(k, to).start()
        gate_copy(near).start()
    for c, j in row_order[held:]:
        row_copy(c, j).start()
    far()
    for c in row_cols:
        gate_copy(c).start()

    earlier = (row_i < col_i).astype(BF16)
    slot_i = lax.broadcasted_iota(jnp.int32, (room, seq), 0)
    gg_copy.wait_recv()
    for c in col_peers:
        send(gg_all.at[z], gg_all.at[z], GGZ, ggzr, exp_peer(c)).start()

    def places(w):
        named = w >= 0.0
        before = mm(jnp.where(named, 1.0, 0.0).astype(BF16), earlier).astype(jnp.int32)
        hits = []
        for j in range(w.shape[0]):
            hits.append(jnp.logical_and(before[j : j + 1] == slot_i, named[j : j + 1]))
        spread = [jnp.where(hit, w[j : j + 1], 0.0).astype(BF16) for j, hit in enumerate(hits)]
        return spread, hits

    def spreads(w):
        return jnp.concatenate(places(jnp.concatenate(by_side(w), axis=0))[0], axis=0)

    def row_wait(c):
        drain(rows.at[c, 1], xr.at[c])

    s_copy = send(s_out, s_in, SHARE, shr, {"exp": partner})

    def share_far():
        diag_copy(0, near).wait_recv()
        far_out[...] = shared(diag_in[...], near)
        far_copy(edge, near).start()

    def share():
        if paired:
            share_far()
        across_copy.wait_recv()
        s_out[...] = shared(across[...], z)
        s_copy.start()

    def part_copy(c):
        return send(p_out.at[c], p_in.at[z], PART, pr.at[z], exp_peer(c))

    spread_z = spreads(gt[z])
    grad_v[...] = mm(spread_z[: local * room], rows[z, 0], TN)
    def slots_to(c, k):
        gate_wait(c).wait_recv()
        spread_v[k] = spreads(gates[c])

    def shared(w, c):
        return mm(jnp.concatenate(places(w)[0], axis=0), row_send[c], TN).astype(BF16)

    def whole_part(c, k):
        row_wait(c)
        p_out[c] = mm(spread_v[k], rows[c].reshape(pair * room, width), TN).astype(BF16)
        part_copy(c).start()

    last = len(row_cols)

    def later_slots():
        for k in range(1, last):
            slots_to(row_cols[k], k)

    low = z < cols // 2
    high = z >= cols // 2
    if row_cols:
        slots_to(row_cols[0], 0)
        whole_part(row_cols[0], 0)
    if paired:
        pl.when(high)(later_slots)
    share()
    if paired:
        pl.when(low)(later_slots)
    else:
        later_slots()
    for k in range(1, last):
        whole_part(row_cols[k], k)
    if paired:
        for k, (on, c) in enumerate(askers):
            @pl.when(on)
            def _():
                near_copy(k, c).wait_recv()
                spread = jnp.concatenate(places(by_side(gt[c])[0])[0], axis=0)
                grad_v[...] = grad_v[...] + mm(spread, near_in[k], TN)
    if cols > 1:
        drain(gg_all.at[pl.ds(0, cols - 1)], ggzr)
    every = jnp.where(member, 1.0, 0.0).astype(BF16)
    order = mm(every, earlier).astype(jnp.int32)
    pick_e = lax.broadcasted_iota(jnp.int32, (experts_all, experts_all * n_exp), 0)
    pick_s = lax.broadcasted_iota(jnp.int32, (experts_all, experts_all * n_exp), 1)
    own_seq = jnp.where(pick_e * n_exp + e == pick_s, 1.0, 0.0).astype(BF16)
    table = mm(own_seq, gg_all[...].reshape(experts_all * n_exp, cap))
    slot_grads = jnp.zeros((experts_all, seq), F32)
    for s in range(cap):
        slot_grads = slot_grads + jnp.where(order == s, table[:, s : s + 1], 0.0)
    weights = jnp.concatenate([jnp.maximum(gt[c], 0.0) for c in range(cols)], axis=0)
    mean = jnp.sum(weights * slot_grads, axis=0, keepdims=True)
    diff = weights * (slot_grads - mean)
    diff_hi = diff.astype(BF16)
    diff_lo = (diff - diff_hi.astype(F32)).astype(BF16)
    grad = grad_v[...] + mm(diff_hi, router_ref[...], TN) + mm(diff_lo, router_ref[...], TN)
    loads["og"].wait()
    loads["scale"].wait()
    scale = jnp.sum(
        jnp.where(row_i == col_i, jnp.broadcast_to(scale_ref[...], (seq, seq)), 0.0),
        axis=1, keepdims=True,
    )
    rows_w = w_v.shape[1]
    tile = min(512, rows_w)
    group = max(rows_w // 2, HEAD_WIDTH)
    per = group // HEAD_WIDTH

    def piece(p, k):
        return (
            jnp.concatenate([gh_all[p, k], x_all[p, :, k * half : (k + 1) * half]], axis=0),
            k * half, half,
        )

    def whole(p):
        return (
            jnp.concatenate(
                [jnp.concatenate([gh_all[p, 0], gh_all[p, 1]], axis=1), x_all[p]], axis=0
            ),
            0, width,
        )

    def product(p, block, r):
        a, at, size = block
        return mm(a, w_v[p, r : r + tile, at : at + size], NT)

    def add_product(p, block):
        for r in range(0, rows_w, tile):
            ctx[:, r : r + tile] = ctx[:, r : r + tile] + product(p, block, r)

    def arrived(p, k):
        for kk in (0, 1) if k is None else (k,):
            drain(gh_all.at[p, kk], hr.at[p, kk])

    def stage(p, k):
        arrived(p, k)
        add_product(p, whole(p) if k is None else piece(p, k))

    drain(w_v, w_sem)
    if n_head > 1:
        drain(x_all.at[pl.ds(0, n_head - 1)], xar)

    s_copy.wait_recv()
    grad = grad + s_in[...].astype(F32)
    if paired:
        grad_v[...] = grad
        for k, (on, to) in enumerate(askers):
            @pl.when(on)
            def _():
                far_copy(k, to).wait_recv()
                grad_v[...] = grad_v[...] + far_in[k].astype(F32)
        grad = grad_v[...]
    if row_cols:
        grad_v[...] = grad
        for c in range(cols):
            beside = c + 1 if c < cols - 1 else c - 1

            @pl.when(jnp.logical_and(z != c, z != beside))
            def _():
                drain(p_in.at[c], pr.at[c])
                grad_v[...] = grad_v[...] + p_in[c].astype(F32)
        grad = grad_v[...]


    def gh_copy(src, k, to):
        return send(
            gh_all.at[src, k], gh_all.at[src, k], GH, hr.at[src, k], {"head": to}
        )

    def half_of(a, k):
        return a[:, k * half : (k + 1) * half]

    def inner_copy(src, to):
        return send(inner_v.at[src], inner_v.at[src], INNER, inr, {"head": to})

    base = []
    for k in range(2):
        base.append(
            half_of(og_ref[...], k).astype(F32) + scale * (half_of(gain, k) * half_of(grad, k))
        )
        gh_all[h, k] = base[k].astype(BF16)
        for p in [sibling] + same:
            gh_copy(h, k, p).start()
        if k == 0:
            inner_v[h] = jnp.broadcast_to(
                jnp.sum(hidden_f32() * gain * grad, axis=1, keepdims=True), (seq, HEAD_WIDTH)
            )
            for p in head_peers:
                inner_copy(h, p).start()
    for k in range(2):
        for p in cross:
            gh_copy(h, k, p).start()
    add_product(h, whole(h))
    if chips > 1:
        stages = [(sibling, None)]
        for p in same + cross:
            stages += [(p, 0), (p, 1)]
    else:
        stages = [(sibling, None)]
    for i, (p, k) in enumerate(stages[:-1]):
        arrived(p, k)
        add_product(p, whole(p) if k is None else piece(p, k))

    if n_head > 1:
        drain(inner_v.at[pl.ds(0, n_head - 1)], inr)
    inner = inner_v[0]
    for i in range(1, n_head):
        inner = inner + inner_v[i]
    taken = scale * inner[:, 0:1] / width_total

    p, k = stages[-1]
    arrived(p, k)
    block = whole(p) if k is None else piece(p, k)
    key_block = k_ref[:, lanes]
    value_block = v_ref[:, lanes]
    gk = jnp.zeros((seq, HEAD_WIDTH), F32)
    gv = jnp.zeros((seq, HEAD_WIDTH), F32)

    def q_copy(r, to):
        at = pl.ds(r, group)
        return send(q_send.at[to, :, at], q_in.at[h, :, at], QS, qr, {"head": to})

    def kv_copy(to):
        return send(kv_send.at[to], kv_in.at[h], KVS, kvr, {"head": to})

    def finish(r):
        for t in range(r, r + group, min(tile, group)):
            size = min(tile, group)
            a, at, depth = block
            ctx[:, t : t + size] = ctx[:, t : t + size] + mm(
                a, w_v[p, t : t + size, at : at + depth], NT
            )

    def back(r):
        part = ctx[:, r : r + group]
        ctx_s = stacked((part[:seq] - taken * part[seq:]).astype(BF16))
        first = r // HEAD_WIDTH
        probs = probs_v[first * seq : (first + per) * seq]
        prob_grads = mm(ctx_s, value_block, NT)
        delta = jnp.sum(probs * prob_grads, axis=1, keepdims=True)
        score_grads = (probs * (prob_grads - delta) * inv_sqrt).astype(BF16)
        gq = mm(score_grads, key_block).astype(BF16)
        for d in range(n_head):
            for i in range(per):
                s = i * seq + d * tok
                q_send[d, :, r + i * HEAD_WIDTH : r + (i + 1) * HEAD_WIDTH] = gq[s : s + tok]
        return score_grads, probs.astype(BF16), ctx_s

    def depart(r):
        for to in head_peers:
            q_copy(r, to).start()

    groups = list(range(0, rows_w, group))
    kept = []
    finish(groups[0])
    for i, r in enumerate(groups):
        kept.append(back(r))
        if i + 1 < len(groups):
            finish(groups[i + 1])
        depart(r)
    for r, (score_grads, probs, ctx_s) in zip(groups, kept):
        gk = gk + mm(score_grads, stacked(q_ref[:, r : r + group]), TN)
        gv = gv + mm(probs, ctx_s, TN)
    for d in range(n_head):
        kv_send[d, 0] = gk[d * tok : (d + 1) * tok].astype(BF16)
        kv_send[d, 1] = gv[d * tok : (d + 1) * tok].astype(BF16)
    for to in head_peers:
        kv_copy(to).start()
    for k in range(2):
        gh_out[:, k * half : (k + 1) * half] = (
            base[k] - half_of(hidden_f32(), k) * taken
        ).astype(BF16)
    q_in[h] = q_send[h]
    kv_in[h] = kv_send[h]

    others = pl.ds(0, n_head - 1)
    some_cols = pl.ds(0, cols - 1)
    sent = []
    if row_cols:
        sent += [
            (row_send.at[pl.ds(0, len(row_cols))], ROWS), (p_out.at[pl.ds(0, len(row_cols))], PART),
        ]
    if paired:
        near_copy(edge, near).wait_send()
        gate_wait(near).wait_recv()
        far_copy(edge, near).wait_send()
        for k, (on, to) in enumerate(askers):
            @pl.when(on)
            def _():
                diag_copy(k, to).wait_send()
    if cols > 1:
        sent += [(gt.at[some_cols], GATE), (gg_all.at[some_cols], GGZ)]
    if n_head > 1:
        sent += [
            (logit.at[others], LOGIT), (x_all.at[others], XALL), (gh_all.at[others], GH),
            (inner_v.at[others], INNER),
        ]
    gg_copy.wait_send()
    across_copy.wait_send()
    s_copy.wait_send()
    for ref, which in sent:
        drain(ref, send_sem.at[which])
    if n_head > 1:
        drain(q_in.at[others], qr)
        drain(kv_in.at[others], kvr)
    span = heads * HEAD_WIDTH
    for i in range(n_head):
        gq_out[:, i * span : (i + 1) * span] = q_in[i]
    replicas = n_head // KEY_VALUE_HEADS
    for g in range(KEY_VALUE_HEADS):
        for k, out in enumerate((gk_out, gv_out)):
            total = kv_in[g * replicas, k].astype(F32)
            for i in range(1, replicas):
                total = total + kv_in[g * replicas + i, k].astype(F32)
            out[:, g * HEAD_WIDTH : (g + 1) * HEAD_WIDTH] = total.astype(BF16)
    if n_head > 1:
        drain(q_send.at[others], send_sem.at[QS])
        drain(kv_send.at[others], send_sem.at[KVS])


def write_out(*refs):
    n = (len(refs) - 1) // 2
    sems = refs[-1]
    copies = [
        pltpu.make_async_copy(refs[i], refs[n + i], sems.at[i]) for i in range(n)
    ]
    for cp in copies:
        cp.start()
    for cp in copies:
        cp.wait()


def solution(mesh):
    n_exp = mesh.shape["exp"]
    n_head = mesh.shape["head"]
    cols = n_exp // 2

    def per_device(
        normed_input, norm_gain, norm_scale, out_grad, router_weight, routed_experts,
        expert_grad, gate_grad, out_proj, query_states, rotated_keys, value_tensor,
    ):
        _, seq, width = normed_input.shape
        experts_all = router_weight.shape[1]
        local, _, cap, _ = expert_grad.shape
        pair = 2 * local
        span, width_total = out_proj.shape
        heads = span // HEAD_WIDTH
        tok = seq // n_head
        kv_width = rotated_keys.shape[2]
        vm = pltpu.VMEM
        dma = pltpu.SemaphoreType.DMA
        vmem = pl.BlockSpec(memory_space=pltpu.VMEM)
        hbm = pl.BlockSpec(memory_space=pltpu.HBM)
        room = -(-cap // 16) * 16
        top_k = routed_experts.shape[2]
        outs = pl.pallas_call(
            functools.partial(kernel, n_exp, n_head, width_total),
            name="moe_attention_backward",
            out_shape=(
                jax.ShapeDtypeStruct((seq, width), BF16),
                jax.ShapeDtypeStruct((tok, n_head * span), BF16),
                jax.ShapeDtypeStruct((tok, kv_width), BF16),
                jax.ShapeDtypeStruct((tok, kv_width), BF16),
            ),
            in_specs=[hbm] * 12,
            out_specs=(vmem,) * 4,
            scratch_shapes=[
                vm((1, width), F32), vm((1, seq), F32),
                vm((seq, width), BF16), vm((experts_all, width), BF16),
                vm((top_k, seq), jnp.int32), vm((local, cap, n_exp, width), BF16),
                vm((cols, 2) + gate_grad.shape, BF16), vm((seq, span), BF16),
                vm((seq, kv_width), BF16), vm((seq, kv_width), BF16), dma((11,)),
                vm((n_head, span, width), BF16),
                vm((cols, local * room, width), BF16),
                vm((cols, 2, local * room, width), BF16),
                vm((n_head, experts_all, seq), F32),
                vm((cols, pair, seq), F32),
                vm((cols, pair, seq), F32),
                vm((cols, seq, width), BF16),
                vm((cols, seq, width), BF16),
                vm((n_head, seq, HEAD_WIDTH), F32),
                vm((n_head, 2, seq, width // 2), BF16),
                vm((n_head, seq, width), BF16),
                vm((2 * seq, span), F32),
                vm((heads * seq, seq), F32),
                vm((n_head, tok, span), BF16),
                vm((n_head, tok, span), BF16),
                vm((n_head, 2, tok, HEAD_WIDTH), BF16),
                vm((n_head, 2, tok, HEAD_WIDTH), BF16),
                vm((local, seq), F32), vm((local, seq), F32),
                vm((seq, width), BF16), vm((seq, width), BF16),
                vm((local, seq), F32), vm((2, local, seq), F32),
                vm((seq, width), BF16), vm((2, seq, width), BF16),
                vm((2, local * room, width), BF16),
                vm((max(cols - 1, 1), pair * room, seq), BF16), vm((seq, width), F32),
                dma, dma((17,)), dma((cols,)), dma, dma, dma((cols,)), dma((cols,)), dma,
                dma, dma((n_head, 2)), dma, dma, dma, dma, dma, dma, dma((2,)), dma((2,)),
                pltpu.SemaphoreType.REGULAR, pltpu.SemaphoreType.REGULAR,
                pltpu.SemaphoreType.REGULAR,
            ],
            compiler_params=pltpu.CompilerParams(
                collective_id=0, has_side_effects=True, vmem_limit_bytes=48 * 1024 * 1024
            ),
        )(
            *(
                pltpu.with_memory_space_constraint(a, pltpu.HBM)
                for a in (
                    normed_input[0], norm_gain[None], norm_scale, out_grad[0], router_weight.T,
                    routed_experts[0].T, jnp.transpose(expert_grad, (0, 2, 1, 3)), gate_grad,
                    out_proj, query_states[0], rotated_keys[0], value_tensor[0],
                )
            )
        )
        outs = pl.pallas_call(
            write_out,
            name="write_out",
            out_shape=tuple(jax.ShapeDtypeStruct(o.shape, o.dtype) for o in outs),
            in_specs=[vmem] * 4,
            out_specs=(hbm,) * 4,
            scratch_shapes=[dma((4,))],
            compiler_params=pltpu.CompilerParams(vmem_limit_bytes=1024 * 1024),
        )(*outs)
        return tuple(o[None] for o in outs)

    placed = (
        P("exp", None, "head"),
        P("head"),
        P("exp", None),
        P("exp", None, "head"),
        P("head", None),
        P("exp", None, None),
        P("exp", None, None, "head"),
        P("exp", None, None),
        P("head", None),
        P("exp", None, "head"),
        P("exp", None, None),
        P("exp", None, None),
    )
    return jax.shard_map(
        per_device,
        mesh=mesh,
        in_specs=placed,
        out_specs=(
            P("exp", None, "head"),
            P("exp", "head", None),
            P("exp", "head", None),
            P("exp", "head", None),
        ),
        check_vma=False,
    )
```
